32 devices in a mesh: dp: 4 (over x, y), seq: 8 (over z, core).
Axes of the slice: x: 2, y: 2, z: 4, core: 2. Of those that a mesh axis runs over, the one named last changes fastest.
Arguments:
- hidden: bfloat16 [65536, 2048], P(('dp', 'seq')), parts along dimension 0
- w_query: bfloat16 [2048, 8, 256], replicated
- w_key: bfloat16 [2048, 8, 256], replicated
- w_value: bfloat16 [2048, 8, 256], replicated
- w_out: bfloat16 [8, 256, 2048], replicated
Outputs:
- output: bfloat16 [65536, 2048], P(('dp', 'seq')), parts along dimension 0
There are 4 independent parts. The reference program is written for one: setup_inputs(seed, part) draws one part's arguments, and reference() takes and returns one part's arrays. A program takes and returns all parts, laid end to end along the dimension named above; an argument that names none is the same for every part.
All inputs are finite; a program needn't handle non-finite values.
Results may differ from the reference program's by a relative error of at most 0.00368.
Values are sent between devices in bfloat16 or wider.
A program may use at most 1 GiB of HBM per device.

```python
import jax
import jax.numpy as jnp
from jax import lax

TOKENS = 16384
D_MODEL = 2048
NUM_HEADS = 8
HEAD_DIM = 256
SEG_BASE = 2048
BRANCHES = 4


def setup_inputs(seed: int = 0, part: int = 0) -> dict:
    base_key = jax.random.key(seed)
    row_key = jax.random.fold_in(jax.random.fold_in(base_key, 1), part)
    weight_keys = jax.random.split(jax.random.fold_in(base_key, 2), 4)
    init_scale = D_MODEL ** -0.5
    out_scale = (SEG_BASE * BRANCHES / (20.0 * D_MODEL)) ** 0.5
    hidden = jax.random.normal(row_key, (TOKENS, D_MODEL), jnp.float32)
    w_query = jax.random.normal(weight_keys[0], (D_MODEL, NUM_HEADS, HEAD_DIM), jnp.float32) * (1.5 * init_scale)
    w_key = jax.random.normal(weight_keys[1], (D_MODEL, NUM_HEADS, HEAD_DIM), jnp.float32) * init_scale
    w_value = jax.random.normal(weight_keys[2], (D_MODEL, NUM_HEADS, HEAD_DIM), jnp.float32) * init_scale
    w_out = jax.random.normal(weight_keys[3], (NUM_HEADS, HEAD_DIM, D_MODEL), jnp.float32) * out_scale
    return {'hidden': hidden.astype(jnp.bfloat16), 'w_query': w_query.astype(jnp.bfloat16), 'w_key': w_key.astype(jnp.bfloat16), 'w_value': w_value.astype(jnp.bfloat16), 'w_out': w_out.astype(jnp.bfloat16)}


def attend_segment(seg_blocks):
    q_seg, k_seg, v_seg = seg_blocks
    n_rows = q_seg.shape[0]
    allowed = jnp.arange(n_rows)[:, None] >= jnp.arange(n_rows)[None, :]
    logits = jnp.dot(q_seg, k_seg.T, preferred_element_type=jnp.float32)
    logits = jnp.where(allowed, logits, -jnp.inf)
    row_max = jnp.max(logits, axis=1, keepdims=True)
    exp_scores = jnp.exp(logits - row_max)
    row_sum = jnp.sum(exp_scores, axis=1)
    weighted = jnp.dot(exp_scores.astype(jnp.bfloat16), v_seg, preferred_element_type=jnp.float32)
    return weighted / row_sum[:, None], row_max[:, 0] + jnp.log(row_sum)


def head_output(head_idx, q_all, k_all, v_all):
    q_head = lax.dynamic_index_in_dim(q_all, head_idx, axis=1, keepdims=False)
    k_head = lax.dynamic_index_in_dim(k_all, head_idx, axis=1, keepdims=False)
    v_head = lax.dynamic_index_in_dim(v_all, head_idx, axis=1, keepdims=False)
    dense_outs = []
    dense_lses = []
    for branch in range(BRANCHES):
        dilation = 2 ** branch
        seg_len = SEG_BASE * dilation
        head_slot = head_idx % dilation
        chosen = jnp.arange(dilation) == head_slot

        def thin_rows(array_in):
            kept_rows = lax.dynamic_index_in_dim(array_in.reshape(TOKENS // dilation, dilation, HEAD_DIM), head_slot, axis=1, keepdims=False)
            return kept_rows.reshape(TOKENS // seg_len, SEG_BASE, HEAD_DIM)

        seg_out, seg_lse = lax.map(attend_segment, (thin_rows(q_head), thin_rows(k_head), thin_rows(v_head)))
        dense_outs.append((seg_out.reshape(TOKENS // dilation, 1, HEAD_DIM) * chosen.astype(jnp.float32)[None, :, None]).reshape(TOKENS, HEAD_DIM))
        dense_lses.append(jnp.where(chosen[None, :], seg_lse.reshape(TOKENS // dilation, 1), -jnp.inf).reshape(TOKENS))
    lse_all = jnp.stack(dense_lses)
    lse_max = jnp.max(lse_all, axis=0)
    branch_weights = jnp.exp(lse_all - lse_max[None, :])
    merged = jnp.sum(branch_weights[:, :, None] * jnp.stack(dense_outs), axis=0) / jnp.sum(branch_weights, axis=0)[:, None]
    return merged.astype(jnp.bfloat16)


def reference(hidden, w_query, w_key, w_value, w_out):
    flat_shape = (D_MODEL, NUM_HEADS * HEAD_DIM)
    head_shape = (TOKENS, NUM_HEADS, HEAD_DIM)
    q_all = (jnp.dot(hidden, w_query.reshape(flat_shape), preferred_element_type=jnp.float32) * HEAD_DIM ** -0.5).astype(jnp.bfloat16).reshape(head_shape)
    k_all = jnp.dot(hidden, w_key.reshape(flat_shape), preferred_element_type=jnp.float32).astype(jnp.bfloat16).reshape(head_shape)
    v_all = jnp.dot(hidden, w_value.reshape(flat_shape), preferred_element_type=jnp.float32).astype(jnp.bfloat16).reshape(head_shape)
    mixed = lax.map(lambda head_idx: head_output(head_idx, q_all, k_all, v_all), jnp.arange(NUM_HEADS))
    attn_out = jnp.einsum('hte,hed->td', mixed.astype(jnp.float32), w_out.astype(jnp.float32))
    return attn_out.astype(jnp.bfloat16)
```

```python
import math
import jax
import jax.numpy as jnp
from jax import lax
from jax.experimental import pallas as pl
from jax.experimental.pallas import tpu as pltpu
from jax.sharding import PartitionSpec as P

CHUNK = 256
CLASSES = 8
RUN = CHUNK // CLASSES
LOG2E = math.log2(math.e)
F32 = jnp.float32
BF16 = jnp.bfloat16
VMEM_LIMIT = 60 * 1024 * 1024


def params():
    return pltpu.CompilerParams(vmem_limit_bytes=VMEM_LIMIT, dimension_semantics=("arbitrary",))


def dot_nt(a, b):
    return lax.dot_general(a, b, (((1,), (1,)), ((), ())), preferred_element_type=F32)


def dot_nn(a, b):
    return lax.dot_general(a, b, (((1,), (0,)), ((), ())), preferred_element_type=F32)


def class_of_group(head, group):
    return head ^ (0, 4, 2, 6)[group]


def run_rows(chunk, cls):
    return pl.ds(pl.multiple_of(chunk * CHUNK + cls * RUN, RUN), RUN)


def gather_class(ref, cls, n_chunks):
    return jnp.concatenate([ref[0, run_rows(i, cls), :] for i in range(n_chunks)], axis=0)


def unpermute_matrix():
    row = lax.broadcasted_iota(jnp.int32, (CHUNK, CHUNK), 0)
    col = lax.broadcasted_iota(jnp.int32, (CHUNK, CHUNK), 1)
    return (row == (col % RUN) * CLASSES + col // RUN).astype(F32).astype(BF16)


def pack_kernel(n_groups, src_ref, *out_refs):
    head = pl.program_id(0)
    n_chunks = src_ref.shape[1] // CHUNK
    rows = n_chunks * RUN
    for group in range(n_groups):
        cls = class_of_group(head, group)
        block = gather_class(src_ref, cls, n_chunks)
        for out_ref in out_refs:
            if out_ref.shape[1] > group * rows:
                out_ref[0, group * rows:(group + 1) * rows, :] = block


def pack(src, group_counts):
    num_heads, tokens, width = src.shape
    rows = tokens // CLASSES
    shapes = [(num_heads, rows * count, width) for count in group_counts]
    spec = lambda shape: pl.BlockSpec((1,) + shape[1:], lambda h: (h, 0, 0))
    return pl.pallas_call(
        lambda *refs: pack_kernel(max(group_counts), *refs),
        grid=(num_heads,),
        out_shape=[jax.ShapeDtypeStruct(s, BF16) for s in shapes],
        in_specs=[spec(src.shape)],
        out_specs=[spec(s) for s in shapes],
        compiler_params=params(),
        cost_estimate=pl.CostEstimate(flops=10 ** 8, bytes_accessed=2 * src.size * 2, transcendentals=0),
        name="pack",
    )(src)


def update(q, blocks, m, l, acc):
    scores = [dot_nt(q, keys) * LOG2E for keys, _, _ in blocks]
    m_new = m
    for s in scores:
        m_new = jnp.maximum(m_new, jnp.max(s, axis=1, keepdims=True))
    alpha = jnp.exp2(m - m_new)
    l = l * alpha
    acc = acc * alpha
    for s, (_, values, log_mult) in zip(scores, blocks):
        p = jnp.exp2(s - (m_new - log_mult))
        l = l + jnp.sum(p, axis=1, keepdims=True)
        acc = acc + dot_nn(p.astype(BF16), values)
    return m_new, l, acc


def local_kernel(flag_ref, q_ref, k_ref, v_ref, pk_ref, pv_ref, o_ref, lse_ref, pat_ref):
    head = pl.program_id(0)
    tokens = q_ref.shape[1]
    n_chunks = tokens // CHUNK
    rows = n_chunks * RUN

    row = lax.broadcasted_iota(jnp.int32, (CHUNK, CHUNK), 0)
    col = lax.broadcasted_iota(jnp.int32, (CHUNK, CHUNK), 1)
    row_x = (row // RUN) ^ head
    col_x = (col // RUN) ^ head
    both = row_x | col_x
    log_mult = jnp.where(both == 0, 2.0, jnp.where(both % 4 == 0, math.log2(3.0), jnp.where(both % 2 == 0, 1.0, 0.0)))
    causal = (row % RUN) * CLASSES + row // RUN >= (col % RUN) * CLASSES + col // RUN
    pat_ref[:, :CHUNK] = log_mult
    pat_ref[:, CHUNK:] = jnp.where(causal, log_mult, -jnp.inf)

    for i in range(n_chunks):
        q = q_ref[0, i * CHUNK:(i + 1) * CHUNK, :]
        scores = []
        m = None
        for j in range(i + 1):
            s = dot_nt(q, k_ref[0, j * CHUNK:(j + 1) * CHUNK, :])
            s = s * LOG2E + (pat_ref[:, CHUNK:] if j == i else pat_ref[:, :CHUNK])
            scores.append(s)
            m = s if m is None else jnp.maximum(m, s)
        m = jnp.max(m, axis=1, keepdims=True)
        total = None
        acc = None
        for j in range(i + 1):
            p = jnp.exp2(scores[j] - m)
            total = p if total is None else total + p
            part = dot_nn(p.astype(BF16), v_ref[0, j * CHUNK:(j + 1) * CHUNK, :])
            acc = part if acc is None else acc + part
        l = jnp.sum(total, axis=1, keepdims=True)
        o_ref[0, i * CHUNK:(i + 1) * CHUNK, :] = acc / l
        lse_ref[0, i * CHUNK:(i + 1) * CHUNK, :] = jnp.broadcast_to(m + jnp.log2(l), (CHUNK, 128))

    mult = ((3, 2, 1, 1), (2, 2, 1, 1), (1, 1, 1, 1), (1, 1, 1, 1))

    @pl.when(flag_ref[0] == 1)
    def _():
        for group in range(4):
            cls = class_of_group(head, group)
            q = gather_class(q_ref, cls, n_chunks)
            acc = gather_class(o_ref, cls, n_chunks)
            m = gather_class(lse_ref, cls, n_chunks)[:, :1]
            blocks = [(pk_ref[0, g * rows:(g + 1) * rows, :], pv_ref[0, g * rows:(g + 1) * rows, :], math.log2(mult[group][g]))
                      for g in range(4)]
            m, l, acc = update(q, blocks, m, jnp.ones_like(m), acc)
            out = acc / l
            lse = jnp.broadcast_to(m + jnp.log2(l), (rows, 128))
            for i in range(n_chunks):
                o_ref[0, run_rows(i, cls), :] = out[i * RUN:(i + 1) * RUN, :]
                lse_ref[0, run_rows(i, cls), :] = lse[i * RUN:(i + 1) * RUN, :]


def head_spec(shape):
    return pl.BlockSpec((1,) + shape[1:], lambda h, flags: (h, 0, 0))


def local_attention(flags, q, k, v, pair_k, pair_v):
    num_heads, tokens, _ = q.shape
    lse_shape = (num_heads, tokens, 128)
    return pl.pallas_call(
        local_kernel,
        grid_spec=pltpu.PrefetchScalarGridSpec(
            num_scalar_prefetch=1,
            grid=(num_heads,),
            in_specs=[head_spec(a.shape) for a in (q, k, v, pair_k, pair_v)],
            out_specs=[head_spec(q.shape), head_spec(lse_shape)],
            scratch_shapes=[pltpu.VMEM((CHUNK, 2 * CHUNK), F32)],
        ),
        out_shape=[jax.ShapeDtypeStruct(q.shape, F32), jax.ShapeDtypeStruct(lse_shape, F32)],
        compiler_params=params(),
        cost_estimate=pl.CostEstimate(flops=4 * 10 ** 10, bytes_accessed=6 * 10 ** 7, transcendentals=3 * 10 ** 7),
        name="local_attention",
    )(flags, q, k, v, pair_k, pair_v)


def far_kernel(flag_ref, qa_ref, qb_ref, *refs):
    keys, values, outs = refs[:4], refs[4:8], refs[8:]

    @pl.when(flag_ref[2] == 1)
    def _():
        for side, q_ref in enumerate((qa_ref, qb_ref)):
            q = q_ref[0]
            scores = [dot_nt(q, k_ref[0]) * LOG2E for k_ref in keys]
            m = jnp.max(jnp.maximum(jnp.maximum(scores[0], scores[1]), jnp.maximum(scores[2], scores[3])), axis=1, keepdims=True)
            probs = [jnp.exp2(s - m) for s in scores]
            l = jnp.sum(probs[0] + probs[1] + probs[2] + probs[3], axis=1, keepdims=True)
            acc = None
            for p, v_ref in zip(probs, values):
                part = dot_nn(p.astype(BF16), v_ref[0])
                acc = part if acc is None else acc + part
            outs[2 * side][0] = acc / l
            lse = jnp.broadcast_to(m + jnp.log2(l), (q.shape[0], 128))
            outs[2 * side + 1][0] = jnp.transpose(lse)[:8, :]


def far_attention(flags, q_own, q_later, keys, values):
    num_heads, rows, _ = q_own.shape
    lse_shape = (num_heads, 8, rows)
    ins = (q_own, q_later, *keys, *values)
    return pl.pallas_call(
        far_kernel,
        grid_spec=pltpu.PrefetchScalarGridSpec(
            num_scalar_prefetch=1,
            grid=(num_heads,),
            in_specs=[head_spec(a.shape) for a in ins],
            out_specs=[head_spec(q_own.shape), head_spec(lse_shape)] * 2,
        ),
        out_shape=[jax.ShapeDtypeStruct(q_own.shape, F32), jax.ShapeDtypeStruct(lse_shape, F32)] * 2,
        compiler_params=params(),
        cost_estimate=pl.CostEstimate(flops=5 * 10 ** 9, bytes_accessed=2 * 10 ** 7, transcendentals=4 * 10 ** 6),
        name="far_attention",
    )(flags, *ins)


def final_kernel(flag_ref, q_ref, o_in_ref, lse_in_ref, k0_ref, k1_ref, v0_ref, v1_ref,
                 fo0_ref, fl0_ref, fo1_ref, fl1_ref, y_ref, o_ref, lse_ref):
    head = pl.program_id(0)
    n_chunks = q_ref.shape[1] // CHUNK
    rows = n_chunks * RUN
    o_ref[...] = o_in_ref[...]
    for group in range(2):
        lse_ref[group * rows:(group + 1) * rows, :] = gather_class(lse_in_ref, class_of_group(head, group), n_chunks)

    def merge(fo_ref, fl_ref):
        cls = class_of_group(head, 0)
        acc = gather_class(o_ref, cls, n_chunks)
        m = lse_ref[:rows, :1]
        lse = fl_ref[0]
        m_far = jnp.transpose(jnp.concatenate([lse] * 16, axis=0))[:, :1]
        m_new = jnp.maximum(m, m_far)
        a, b = jnp.exp2(m - m_new), jnp.exp2(m_far - m_new)
        total = a + b
        out = (acc * a + fo_ref[0] * b) / total
        lse_ref[:rows, :] = jnp.broadcast_to(m_new + jnp.log2(total), (rows, 128))
        for i in range(n_chunks):
            o_ref[0, run_rows(i, cls), :] = out[i * RUN:(i + 1) * RUN, :]

    @pl.when(flag_ref[2] == 1)
    def _():
        merge(fo0_ref, fl0_ref)

    @pl.when(flag_ref[3] == 1)
    def _():
        merge(fo1_ref, fl1_ref)

    mult = ((2, 1), (1, 1))

    @pl.when(flag_ref[1] == 1)
    def _():
        for group in range(2):
            cls = class_of_group(head, group)
            q = gather_class(q_ref, cls, n_chunks)
            acc = gather_class(o_ref, cls, n_chunks)
            m = lse_ref[group * rows:(group + 1) * rows, :1]
            blocks = [(k_ref[0, g * rows:(g + 1) * rows, :], v_ref[0, g * rows:(g + 1) * rows, :], math.log2(mult[group][g]))
                      for k_ref, v_ref in ((k0_ref, v0_ref), (k1_ref, v1_ref)) for g in range(2)]
            m, l, acc = update(q, blocks, m, jnp.ones_like(m), acc)
            out = acc / l
            for i in range(n_chunks):
                o_ref[0, run_rows(i, cls), :] = out[i * RUN:(i + 1) * RUN, :]

    back = unpermute_matrix()
    for i in range(n_chunks):
        part = o_ref[0, i * CHUNK:(i + 1) * CHUNK, :].astype(BF16)
        y_ref[i * CHUNK:(i + 1) * CHUNK, :] = dot_nn(back, part).astype(BF16)


def final_attention(flags, q, o, lse, keys, values, far):
    num_heads, tokens, width = q.shape
    ins = (q, o, lse, *keys, *values, *far)
    return pl.pallas_call(
        final_kernel,
        grid_spec=pltpu.PrefetchScalarGridSpec(
            num_scalar_prefetch=1,
            grid=(num_heads,),
            in_specs=[head_spec(a.shape) for a in ins],
            out_specs=pl.BlockSpec((tokens, width), lambda h, flags: (0, h)),
            scratch_shapes=[pltpu.VMEM((1, tokens, width), F32), pltpu.VMEM((2 * tokens // CLASSES, 128), F32)],
        ),
        out_shape=jax.ShapeDtypeStruct((tokens, num_heads * width), BF16),
        compiler_params=params(),
        cost_estimate=pl.CostEstimate(flops=8 * 10 ** 9, bytes_accessed=6 * 10 ** 7, transcendentals=5 * 10 ** 6),
        name="final_attention",
    )(flags, *ins)


def solution(mesh):
    row_spec = P(('dp', 'seq'), None)
    pair_up = [(s, s + 1) for s in (0, 2, 4, 6)]
    next_chip = [(0, 2), (1, 3), (4, 6), (5, 7)]
    swap_upper = [(s, s ^ 1) for s in (2, 3, 6, 7)]
    from_first = [(0, 4), (1, 5)]
    from_second = [(2, 4), (3, 5)]
    swap_third = [(4, 5), (5, 4)]
    to_third = [(6, 4), (7, 5)]
    to_fourth = [(4, 6), (5, 7)]

    def send(array, pairs):
        return lax.ppermute(array, 'seq', pairs)

    def layer(hidden, w_query, w_key, w_value, w_out):
        tokens, d_model = hidden.shape
        num_heads, head_dim = w_query.shape[1:]
        index = lax.axis_index('seq')
        chip = index // 2
        flags = jnp.stack([index % 2, chip % 2, (chip == 2).astype(jnp.int32), (chip == 3).astype(jnp.int32)]).astype(jnp.int32)

        order = jnp.arange(CHUNK)
        perm = ((order % RUN) * CLASSES + order // RUN)[:, None] == order[None, :]
        x = jnp.einsum('pq,cqd->cpd', perm.astype(BF16), hidden.reshape(tokens // CHUNK, CHUNK, d_model),
                       preferred_element_type=F32).astype(BF16).reshape(tokens, d_model)

        def project(weight):
            return jnp.einsum('td,dhe->hte', x, weight, preferred_element_type=F32)

        def spread(packs):
            far_rows, quad_rows, pair_rows = packs
            first = send(far_rows, from_first)
            second = send(far_rows, from_second)
            quad = send(quad_rows, next_chip)
            pair = send(pair_rows, pair_up)
            swapped = send(first, swap_third), send(second, swap_third)
            return pair, (quad, send(quad, swap_upper)), (first, second, *swapped)

        k = project(w_key).astype(BF16)
        pair_k, quad_k, far_k = spread(pack(k, (1, 2, 4)))
        v = project(w_value).astype(BF16)
        pair_v, quad_v, far_v = spread(pack(v, (1, 2, 4)))
        q = (project(w_query) * head_dim ** -0.5).astype(BF16)
        q_far, = pack(q, (1,))
        q_later = send(q_far, to_third)

        o, lse = local_attention(flags, q, k, v, pair_k, pair_v)
        own_o, own_lse, later_o, later_lse = far_attention(flags, q_far, q_later, far_k, far_v)
        got_o, got_lse = send(later_o, to_fourth), send(later_lse, to_fourth)
        mixed = final_attention(flags, q, o, lse, quad_k, quad_v, (own_o, own_lse, got_o, got_lse))
        return jnp.dot(mixed, w_out.reshape(num_heads * head_dim, d_model), preferred_element_type=F32).astype(BF16)

    return jax.shard_map(layer, mesh=mesh, in_specs=(row_spec, P(), P(), P(), P()), out_specs=row_spec, check_vma=False)
```

```python
import math
import jax
import jax.numpy as jnp
from jax import lax
from jax.experimental import pallas as pl
from jax.experimental.pallas import tpu as pltpu
from jax.sharding import PartitionSpec as P

CHUNK = 256
CLASSES = 8
RUN = CHUNK // CLASSES
LOG2E = math.log2(math.e)
F32 = jnp.float32
BF16 = jnp.bfloat16
VMEM_LIMIT = 60 * 1024 * 1024


def params():
    return pltpu.CompilerParams(vmem_limit_bytes=VMEM_LIMIT, dimension_semantics=("arbitrary",))


def dot_nt(a, b):
    return lax.dot_general(a, b, (((1,), (1,)), ((), ())), preferred_element_type=F32)


def dot_nn(a, b):
    return lax.dot_general(a, b, (((1,), (0,)), ((), ())), preferred_element_type=F32)


def class_of_group(head, group):
    return head ^ (0, 4, 2, 6)[group]


def run_rows(chunk, cls):
    return pl.ds(pl.multiple_of(chunk * CHUNK + cls * RUN, RUN), RUN)


def gather_class(ref, cls, n_chunks):
    return jnp.concatenate([ref[0, run_rows(i, cls), :] for i in range(n_chunks)], axis=0)


def gather_tile(ref, pair, classes):
    return jnp.concatenate([ref[0, run_rows(2 * pair + b, cls), :] for cls in classes for b in range(2)], axis=0)


def lane_class(lane):
    group = lane // (2 * RUN)
    return (group % 2) * 4 + (group // 2) * 2


def lane_position(lane, first_class):
    return (lane // RUN) % 2 * CHUNK + lane % RUN * CLASSES + (lane_class(lane) ^ first_class)


def fold_rows(x, op):
    while x.shape[0] > 8:
        half = x.shape[0] // 2
        x = op(x[:half], x[half:])
    return x


def pack_kernel(n_groups, src_ref, *out_refs):
    head = pl.program_id(0)
    n_chunks = src_ref.shape[1] // CHUNK
    rows = n_chunks * RUN
    for group in range(n_groups):
        cls = class_of_group(head, group)
        block = gather_class(src_ref, cls, n_chunks)
        for out_ref in out_refs:
            if out_ref.shape[1] > group * rows:
                out_ref[0, group * rows:(group + 1) * rows, :] = block


def pack_query_kernel(src_ref, far_ref, late_ref):
    head = pl.program_id(0)
    far_ref[0] = gather_class(src_ref, head, src_ref.shape[1] // CHUNK)
    late = [gather_tile(src_ref, pair, [class_of_group(head, g) for g in range(2)]) for pair in range(src_ref.shape[1] // (2 * CHUNK))]
    late_ref[0] = jnp.concatenate(late, axis=0)


def pack_query(src):
    num_heads, tokens, width = src.shape
    shapes = [(num_heads, tokens // CLASSES, width), (num_heads, tokens // 4, width)]
    spec = lambda shape: pl.BlockSpec((1,) + shape[1:], lambda h: (h, 0, 0))
    return pl.pallas_call(
        pack_query_kernel,
        grid=(num_heads,),
        out_shape=[jax.ShapeDtypeStruct(s, BF16) for s in shapes],
        in_specs=[spec(src.shape)],
        out_specs=[spec(s) for s in shapes],
        compiler_params=params(),
        cost_estimate=pl.CostEstimate(flops=10 ** 8, bytes_accessed=3 * src.size, transcendentals=0),
        name="pack_query",
    )(src)


def pack(src, group_counts):
    num_heads, tokens, width = src.shape
    rows = tokens // CLASSES
    shapes = [(num_heads, rows * count, width) for count in group_counts]
    spec = lambda shape: pl.BlockSpec((1,) + shape[1:], lambda h: (h, 0, 0))
    return pl.pallas_call(
        lambda *refs: pack_kernel(max(group_counts), *refs),
        grid=(num_heads,),
        out_shape=[jax.ShapeDtypeStruct(s, BF16) for s in shapes],
        in_specs=[spec(src.shape)],
        out_specs=[spec(s) for s in shapes],
        compiler_params=params(),
        cost_estimate=pl.CostEstimate(flops=10 ** 8, bytes_accessed=2 * src.size * 2, transcendentals=0),
        name="pack",
    )(src)


def head_spec(shape, first=0, last=None):
    if last is None:
        return pl.BlockSpec((1,) + shape[1:], lambda h, flags: (h + first, 0, 0))
    return pl.BlockSpec((1,) + shape[1:], lambda h, flags: (jnp.minimum(h, last), 0, 0))


def local_kernel(first_head, flag_ref, q_ref, k_ref, v_ref, pk_ref, pv_ref, *refs):
    ot_ref, st_ref, lse_ref, vt_ref, s_ref = refs[-5:]
    head = pl.program_id(0) + first_head
    tokens = q_ref.shape[1]
    n_pairs = tokens // (2 * CHUNK)
    vt_ref[:, :tokens] = jnp.transpose(v_ref[0])
    vt_ref[:, tokens:] = jnp.transpose(pv_ref[0])

    lane = lax.broadcasted_iota(jnp.int32, (8, CHUNK), 1)
    row = lax.broadcasted_iota(jnp.int32, (8, CHUNK), 0)
    both = (row ^ head) | lane_class(lane)
    log_mult = jnp.where(both == 0, 2.0, jnp.where(both % 4 == 0, math.log2(3.0), jnp.where(both % 2 == 0, 1.0, 0.0)))
    both = lane_class(row * 2 * RUN) | lane_class(lane)
    log_mult_pair = jnp.where(both == 0, math.log2(3.0), jnp.where(both % 4 == 0, 1.0, 0.0))
    log_mult_pair = jnp.where(flag_ref[0] == 1, log_mult_pair, -jnp.inf)
    row_run = lax.broadcasted_iota(jnp.int32, (RUN, CHUNK), 0) * CLASSES
    lane_run = lax.broadcasted_iota(jnp.int32, (RUN, CHUNK), 1)

    def scores(tile):
        matched, pair, slot = tile
        first = head if matched else head ^ 1
        q = gather_tile(q_ref, pair, [class_of_group(first, g) for g in range(4)])
        limit = lane_position(lane_run, first) - row_run
        m = jnp.full((8, CHUNK), -jnp.inf, F32)
        for j in range(2 * pair + 2):
            s = dot_nt(k_ref[0, j * CHUNK:(j + 1) * CHUNK, :], q)
            for r in range(CLASSES):
                part = s[r * RUN:(r + 1) * RUN, :] * LOG2E
                if matched:
                    part = part + log_mult[r:r + 1, :]
                if j >= 2 * pair:
                    part = jnp.where(limit >= (j - 2 * pair) * CHUNK + r, part, -jnp.inf)
                s_ref[slot, j * CHUNK + r * RUN:j * CHUNK + (r + 1) * RUN, :] = part
                m = jnp.maximum(m, fold_rows(part, jnp.maximum))
        if matched:
            for g in range(4):
                s = dot_nt(pk_ref[0, g * CHUNK:(g + 1) * CHUNK, :], q) * LOG2E + log_mult_pair[g:g + 1, :]
                s_ref[slot, tokens + g * CHUNK:tokens + (g + 1) * CHUNK, :] = s
                m = jnp.maximum(m, fold_rows(s, jnp.maximum))
        return jnp.max(m, axis=0, keepdims=True)

    def values(tile, m):
        matched, pair, slot = tile
        starts = [j * CHUNK for j in range(2 * pair + 2)] + ([tokens + g * CHUNK for g in range(4)] if matched else [])
        total = jnp.zeros((8, CHUNK), F32)
        acc = None
        for start in starts:
            p = jnp.exp2(s_ref[slot, start:start + CHUNK, :] - m)
            total = total + fold_rows(p, jnp.add)
            part = dot_nn(vt_ref[:, start:start + CHUNK], p.astype(BF16))
            acc = part if acc is None else acc + part
        l = jnp.sum(total, axis=0, keepdims=True)
        out = acc * (1.0 / l)
        lanes = (2 * pair + (0 if matched else 1)) * CHUNK
        ot_ref[0, :, lanes:lanes + CHUNK] = out.astype(BF16)
        if matched:
            st_ref[0, :, pair * 128:(pair + 1) * 128] = out[:, :128]
            lse_ref[0, :, pair * 128:(pair + 1) * 128] = jnp.broadcast_to((m + jnp.log2(l))[:, :128], (8, 128))

    tiles = [(matched, pair) for pair in range(n_pairs) for matched in (True, False)]
    tiles = [(matched, pair, n % 2) for n, (matched, pair) in enumerate(tiles)]
    m = scores(tiles[0])
    for tile, following in zip(tiles, tiles[1:] + [None]):
        m_following = None if following is None else scores(following)
        values(tile, m)
        m = m_following


def local_attention(flags, q, k, v, pair_k, pair_v, first_head, count, previous, after):
    num_heads, tokens, width = q.shape
    shapes = [jax.ShapeDtypeStruct((num_heads, width, tokens), BF16),
              jax.ShapeDtypeStruct((num_heads, width, tokens // 4), F32),
              jax.ShapeDtypeStruct((num_heads, 8, tokens // 4), F32)]
    ins = (q, k, v, pair_k, pair_v)
    extra = tuple(previous) + tuple(after)
    return pl.pallas_call(
        lambda *refs: local_kernel(first_head, *refs),
        grid_spec=pltpu.PrefetchScalarGridSpec(
            num_scalar_prefetch=1,
            grid=(count,),
            in_specs=[head_spec(a.shape, first_head) for a in ins] + [pl.BlockSpec(memory_space=pl.ANY)] * len(extra),
            out_specs=[head_spec(s.shape, first_head) for s in shapes],
            scratch_shapes=[pltpu.VMEM((width, tokens + pair_k.shape[1]), BF16),
                            pltpu.VMEM((2, tokens + pair_k.shape[1], CHUNK), F32)],
        ),
        out_shape=shapes,
        input_output_aliases={len(ins) + 1 + n: n for n in range(len(previous))},
        compiler_params=params(),
        cost_estimate=pl.CostEstimate(flops=count * 5 * 10 ** 9, bytes_accessed=count * 10 ** 7, transcendentals=count * 4 * 10 ** 6),
        name="local_attention",
    )(flags, *ins, *extra)


def far_kernel(flag_ref, qa_ref, qb_ref, *refs):
    keys, values, outs = refs[:4], refs[4:8], refs[-4:]
    turned = [jnp.transpose(v_ref[0]) for v_ref in values]
    for side, q_ref in enumerate((qa_ref, qb_ref)):
        scores = [dot_nt(k_ref[0], q_ref[0]) * LOG2E for k_ref in keys]
        m = fold_rows(scores[0], jnp.maximum)
        for s in scores[1:]:
            m = jnp.maximum(m, fold_rows(s, jnp.maximum))
        m = jnp.max(m, axis=0, keepdims=True)
        total = jnp.zeros((8, CHUNK), F32)
        acc = None
        for s, vt in zip(scores, turned):
            p = jnp.exp2(s - m)
            total = total + fold_rows(p, jnp.add)
            part = dot_nn(vt, p.astype(BF16))
            acc = part if acc is None else acc + part
        l = jnp.sum(total, axis=0, keepdims=True)
        outs[2 * side][0] = acc * (1.0 / l)
        outs[2 * side + 1][0] = jnp.broadcast_to(m + jnp.log2(l), (8, CHUNK))


def far_attention(flags, q_own, q_later, keys, values, after):
    num_heads, rows, width = q_own.shape
    shapes = [jax.ShapeDtypeStruct((num_heads, width, rows), F32), jax.ShapeDtypeStruct((num_heads, 8, rows), F32)] * 2
    ins = (q_own, q_later, *keys, *values)
    return pl.pallas_call(
        far_kernel,
        grid_spec=pltpu.PrefetchScalarGridSpec(
            num_scalar_prefetch=1,
            grid=(num_heads,),
            in_specs=[head_spec(a.shape) for a in ins] + [pl.BlockSpec(memory_space=pl.ANY)] * len(after),
            out_specs=[head_spec(s.shape) for s in shapes],
        ),
        out_shape=shapes,
        compiler_params=params(),
        cost_estimate=pl.CostEstimate(flops=5 * 10 ** 9, bytes_accessed=2 * 10 ** 7, transcendentals=4 * 10 ** 6),
        name="far_attention",
    )(flags, *ins, *after)


def final_kernel(num_heads, flag_ref, q_ref, ot_ref, st_ref, lse_ref, k0_ref, k1_ref, v0_ref, v1_ref,
                 fo0_ref, fl0_ref, fo1_ref, fl1_ref, wo_ref, y_ref, o_ref):
    step = pl.program_id(0)

    @pl.when(step < num_heads)
    def _():
        head = step
        lane = lax.broadcasted_iota(jnp.int32, (8, CHUNK), 1)
        first = (lane % 128) < 64
        quad_on = jnp.where(flag_ref[1] == 1, 0.0, -jnp.inf)
        mult_a = jnp.where(first, 1.0, 0.0) + quad_on
        mult_b = jnp.zeros((8, CHUNK), F32) + quad_on
        own_on = jnp.where(flag_ref[2] == 1, 0.0, -jnp.inf)
        got_on = jnp.where(flag_ref[3] == 1, 0.0, -jnp.inf)
        far_lse = jnp.maximum(fl0_ref[0] + own_on, fl1_ref[0] + got_on)
        turned = [jnp.transpose(v_ref[0]) for v_ref in (v0_ref, v1_ref)]
        merged = []
        for half in range(2):
            lanes = slice(half * CHUNK, (half + 1) * CHUNK)
            q = q_ref[0, lanes, :]
            block = slice(half * 128, (half + 1) * 128)
            far = jnp.where(flag_ref[2] == 1, fo0_ref[0, :, block], fo1_ref[0, :, block])
            far = jnp.concatenate([far, pltpu.roll(far, 64, 1)], axis=1)
            f_lse = far_lse[:, block]
            f_lse = jnp.where(first, jnp.concatenate([f_lse, pltpu.roll(f_lse, 64, 1)], axis=1), -jnp.inf)
            lse = lse_ref[0, :, lanes]
            m = jnp.maximum(lse, f_lse)
            scores = []
            for k_ref in (k0_ref, k1_ref):
                for g, mult in enumerate((mult_a, mult_b)):
                    s = dot_nt(k_ref[0, g * CHUNK:(g + 1) * CHUNK, :], q) * LOG2E + mult[:1, :]
                    scores.append(s)
                    m = jnp.maximum(m, fold_rows(s, jnp.maximum))
            m = jnp.max(m, axis=0, keepdims=True)
            total = jnp.zeros((8, CHUNK), F32)
            acc = None
            for n, s in enumerate(scores):
                p = jnp.exp2(s - m)
                total = total + fold_rows(p, jnp.add)
                part = dot_nn(turned[n // 2][:, n % 2 * CHUNK:(n % 2 + 1) * CHUNK], p.astype(BF16))
                acc = part if acc is None else acc + part
            own_weight = jnp.exp2(lse[:1, :] - m)
            far_weight = jnp.exp2(f_lse[:1, :] - m)
            l = jnp.sum(total, axis=0, keepdims=True) + own_weight + far_weight
            out = (acc + st_ref[0, :, lanes] * own_weight + far * far_weight) * (1.0 / l)
            merged.append(out.astype(BF16))

        token = lax.broadcasted_iota(jnp.int32, (2 * CHUNK, CHUNK), 0)
        column = lax.broadcasted_iota(jnp.int32, (2 * CHUNK, CHUNK), 1)
        places = [(token == lane_position(column, c)).astype(F32).astype(BF16) for c in (head, head ^ 1)]
        for pair in range(4):
            start = 2 * pair * CHUNK
            matched = jnp.concatenate([merged[pair // 2][:, pair % 2 * 128:(pair % 2 + 1) * 128],
                                       ot_ref[0, :, start + 128:start + CHUNK]], axis=1)
            rows = dot_nt(places[0], matched) + dot_nt(places[1], ot_ref[0, :, start + CHUNK:start + 2 * CHUNK])
            columns = pl.ds(pl.multiple_of(head * CHUNK, CHUNK), CHUNK)
            o_ref[start:start + 2 * CHUNK, columns] = rows.astype(BF16)

    @pl.when(step >= num_heads)
    def _():
        y_ref[...] = dot_nn(o_ref[...], wo_ref[...]).astype(BF16)


def final_attention(flags, q, ot, st, lse, keys, values, far, w_out):
    num_heads, width, tokens = ot.shape
    d_model = w_out.shape[1]
    ins = (q, ot, st, lse, *keys, *values, *far)
    column = lambda h, flags: (0, jnp.maximum(h - num_heads, 0))
    return pl.pallas_call(
        lambda *refs: final_kernel(num_heads, *refs),
        grid_spec=pltpu.PrefetchScalarGridSpec(
            num_scalar_prefetch=1,
            grid=(num_heads + d_model // 256,),
            in_specs=[head_spec(a.shape, last=num_heads - 1) for a in ins] + [pl.BlockSpec((w_out.shape[0], 256), column)],
            out_specs=pl.BlockSpec((tokens, 256), column),
            scratch_shapes=[pltpu.VMEM((tokens, num_heads * width), BF16)],
        ),
        out_shape=jax.ShapeDtypeStruct((tokens, d_model), BF16),
        compiler_params=params(),
        cost_estimate=pl.CostEstimate(flops=3 * 10 ** 10, bytes_accessed=6 * 10 ** 7, transcendentals=5 * 10 ** 6),
        name="final_attention",
    )(flags, *ins, w_out)


def solution(mesh):
    row_spec = P(('dp', 'seq'), None)
    pair_up = [(s, s + 1) for s in (0, 2, 4, 6)]
    next_chip = [(0, 2), (1, 3), (4, 6), (5, 7)]
    swap_upper = [(s, s ^ 1) for s in (2, 3, 6, 7)]
    from_first = [(0, 4), (1, 5)]
    from_second = [(2, 4), (3, 5)]
    swap_third = [(4, 5), (5, 4)]
    to_third = [(6, 4), (7, 5)]
    to_fourth = [(4, 6), (5, 7)]

    def send(array, pairs):
        return lax.ppermute(array, 'seq', pairs)

    def layer(hidden, w_query, w_key, w_value, w_out):
        tokens, d_model = hidden.shape
        num_heads, head_dim = w_query.shape[1:]
        index = lax.axis_index('seq')
        chip = index // 2
        flags = jnp.stack([index % 2, chip % 2, (chip == 2).astype(jnp.int32), (chip == 3).astype(jnp.int32)]).astype(jnp.int32)

        order = jnp.arange(CHUNK)
        perm = ((order % RUN) * CLASSES + order // RUN)[:, None] == order[None, :]
        x = jnp.einsum('pq,cqd->cpd', perm.astype(BF16), hidden.reshape(tokens // CHUNK, CHUNK, d_model),
                       preferred_element_type=F32).astype(BF16).reshape(tokens, d_model)

        def project(weight):
            return jnp.einsum('td,dhe->hte', x, weight, preferred_element_type=F32)

        def spread(packs):
            far_rows, quad_rows, pair_rows = packs
            first = send(far_rows, from_first)
            second = send(far_rows, from_second)
            quad = send(quad_rows, next_chip)
            pair = send(pair_rows, pair_up)
            swapped = send(first, swap_third), send(second, swap_third)
            return pair, (quad, send(quad, swap_upper)), (first, second, *swapped)

        k = project(w_key).astype(BF16)
        pair_k, quad_k, far_k = spread(pack(k, (1, 2, 4)))
        v = project(w_value).astype(BF16)
        pair_v, quad_v, far_v = spread(pack(v, (1, 2, 4)))
        q = (project(w_query) * head_dim ** -0.5).astype(BF16)
        q_far, q_late = pack_query(q)
        q_later = send(q_far, to_third)

        half = num_heads // 2
        state = local_attention(flags, q, k, v, pair_k, pair_v, 0, half, (), ())
        own_o, own_lse, later_o, later_lse = far_attention(flags, q_far, q_later, far_k, far_v, (state[2],))
        got_o, got_lse = send(later_o, to_fourth), send(later_lse, to_fourth)
        ot, st, lse = local_attention(flags, q, k, v, pair_k, pair_v, half, half, state, (own_lse,))
        return final_attention(flags, q_late, ot, st, lse, quad_k, quad_v, (own_o, own_lse, got_o, got_lse),
                               w_out.reshape(num_heads * head_dim, d_model))

    return jax.shard_map(layer, mesh=mesh, in_specs=(row_spec, P(), P(), P(), P()), out_specs=row_spec, check_vma=False)
```

```python
import math
import jax
import jax.numpy as jnp
from jax import lax
from jax.experimental import pallas as pl
from jax.experimental.pallas import tpu as pltpu
from jax.sharding import PartitionSpec as P

CHUNK = 256
CLASSES = 8
RUN = CHUNK // CLASSES
LOG2E = math.log2(math.e)
F32 = jnp.float32
BF16 = jnp.bfloat16
VMEM_LIMIT = 60 * 1024 * 1024


def params():
    return pltpu.CompilerParams(vmem_limit_bytes=VMEM_LIMIT, dimension_semantics=("arbitrary",))


def dot_nt(a, b):
    return lax.dot_general(a, b, (((1,), (1,)), ((), ())), preferred_element_type=F32)


def dot_nn(a, b):
    return lax.dot_general(a, b, (((1,), (0,)), ((), ())), preferred_element_type=F32)


def class_of_group(head, group):
    return head ^ (0, 4, 2, 6)[group]


def run_rows(chunk, cls):
    return pl.ds(pl.multiple_of(chunk * CHUNK + cls * RUN, RUN), RUN)


def gather_tile(ref, pair, classes):
    return jnp.concatenate([ref[0, run_rows(2 * pair + b, cls), :] for cls in classes for b in range(2)], axis=0)


def lane_class(lane):
    group = lane // (2 * RUN)
    return (group % 2) * 4 + (group // 2) * 2


def lane_position(lane, first_class):
    return (lane // RUN) % 2 * CHUNK + lane % RUN * CLASSES + (lane_class(lane) ^ first_class)


def fold_rows(x, op):
    while x.shape[0] > 8:
        half = x.shape[0] // 2
        x = op(x[:half], x[half:])
    return x


def pack_kernel(n_groups, *refs):
    src_refs, out_refs = refs[:n_groups], refs[n_groups:]
    for group, src_ref in enumerate(src_refs):
        rows = src_ref.shape[1] * RUN
        block = src_ref[...].reshape(rows, src_ref.shape[-1])
        for out_ref in out_refs:
            if out_ref.shape[1] > group * rows:
                out_ref[0, group * rows:(group + 1) * rows, :] = block


def pack(src, group_counts):
    num_heads, tokens, width = src.shape
    n_chunks = tokens // CHUNK
    shapes = [(num_heads, tokens // CLASSES * count, width) for count in group_counts]
    n_groups = max(group_counts)
    runs = src.reshape(num_heads, n_chunks, CLASSES, RUN, width)

    def run_spec(group):
        return pl.BlockSpec((1, n_chunks, 1, RUN, width), lambda h: (h, 0, class_of_group(h, group), 0, 0))

    return pl.pallas_call(
        lambda *refs: pack_kernel(n_groups, *refs),
        grid=(num_heads,),
        out_shape=[jax.ShapeDtypeStruct(s, BF16) for s in shapes],
        in_specs=[run_spec(group) for group in range(n_groups)],
        out_specs=[pl.BlockSpec((1,) + s[1:], lambda h: (h, 0, 0)) for s in shapes],
        compiler_params=params(),
        cost_estimate=pl.CostEstimate(flops=10 ** 8, bytes_accessed=3 * src.size, transcendentals=0),
        name="pack",
    )(*[runs] * n_groups)


def sort_kernel(x_ref, y_ref):
    row = lax.broadcasted_iota(jnp.int32, (CHUNK, CHUNK), 0)
    col = lax.broadcasted_iota(jnp.int32, (CHUNK, CHUNK), 1)
    perm = (col == (row % RUN) * CLASSES + row // RUN).astype(F32).astype(BF16)
    y_ref[...] = dot_nn(perm, x_ref[...]).astype(BF16)


def sort_by_class(x):
    tokens, width = x.shape
    spec = pl.BlockSpec((CHUNK, width), lambda i: (i, 0))
    return pl.pallas_call(
        sort_kernel,
        grid=(tokens // CHUNK,),
        out_shape=jax.ShapeDtypeStruct(x.shape, BF16),
        in_specs=[spec],
        out_specs=spec,
        compiler_params=params(),
        cost_estimate=pl.CostEstimate(flops=2 * 10 ** 9, bytes_accessed=4 * x.size, transcendentals=0),
        name="sort_by_class",
    )(x)


def head_spec(shape, first=0, last=None):
    if last is None:
        return pl.BlockSpec((1,) + shape[1:], lambda h, flags: (h + first, 0, 0))
    return pl.BlockSpec((1,) + shape[1:], lambda h, flags: (jnp.minimum(h, last), 0, 0))


def local_kernel(first_head, flag_ref, q_ref, k_ref, v_ref, pk_ref, pv_ref, *refs):
    ot_ref, st_ref, lse_ref, late_ref, vt_ref, s_ref = refs[-6:]
    head = pl.program_id(0) + first_head
    tokens = q_ref.shape[1]
    n_pairs = tokens // (2 * CHUNK)
    vt_ref[:, :tokens] = jnp.transpose(v_ref[0])
    vt_ref[:, tokens:] = jnp.transpose(pv_ref[0])

    lane = lax.broadcasted_iota(jnp.int32, (8, CHUNK), 1)
    row = lax.broadcasted_iota(jnp.int32, (8, CHUNK), 0)
    both = (row ^ head) | lane_class(lane)
    log_mult = jnp.where(both == 0, 2.0, jnp.where(both % 4 == 0, math.log2(3.0), jnp.where(both % 2 == 0, 1.0, 0.0)))
    both = lane_class(row * 2 * RUN) | lane_class(lane)
    log_mult_pair = jnp.where(both == 0, math.log2(3.0), jnp.where(both % 4 == 0, 1.0, 0.0))
    log_mult_pair = jnp.where(flag_ref[0] == 1, log_mult_pair, -jnp.inf)
    row_run = lax.broadcasted_iota(jnp.int32, (RUN, CHUNK), 0) * CLASSES
    lane_run = lax.broadcasted_iota(jnp.int32, (RUN, CHUNK), 1)

    def scores(tile):
        matched, pair, slot = tile
        first = head if matched else head ^ 1
        q = gather_tile(q_ref, pair, [class_of_group(first, g) for g in range(4)])
        if matched:
            late_ref[0, pair * 128:(pair + 1) * 128, :] = q[:128, :]
        limit = lane_position(lane_run, first) - row_run
        m = jnp.full((8, CHUNK), -jnp.inf, F32)
        for j in range(2 * pair + 2):
            s = dot_nt(k_ref[0, j * CHUNK:(j + 1) * CHUNK, :], q)
            for r in range(CLASSES):
                part = s[r * RUN:(r + 1) * RUN, :]
                if j >= 2 * pair:
                    part = jnp.where(limit >= (j - 2 * pair) * CHUNK + r, part, -jnp.inf)
                s_ref[slot, j * CHUNK + r * RUN:j * CHUNK + (r + 1) * RUN, :] = part
                m = jnp.maximum(m, fold_rows(part, jnp.maximum))
        if matched:
            m_pair = jnp.full((8, CHUNK), -jnp.inf, F32)
            for g in range(4):
                s = dot_nt(pk_ref[0, g * CHUNK:(g + 1) * CHUNK, :], q)
                s_ref[slot, tokens + g * CHUNK:tokens + (g + 1) * CHUNK, :] = s
                m_pair = jnp.maximum(m_pair, fold_rows(s, jnp.maximum))
            m = jnp.maximum(m, jnp.where(flag_ref[0] == 1, m_pair, -jnp.inf))
        return jnp.max(m, axis=0, keepdims=True) * LOG2E

    def values(tile, m):
        matched, pair, slot = tile
        starts = [j * CHUNK for j in range(2 * pair + 2)] + ([tokens + g * CHUNK for g in range(4)] if matched else [])
        total = jnp.zeros((8, CHUNK), F32)
        acc = None
        for start in starts:
            if not matched:
                p = jnp.exp2(s_ref[slot, start:start + CHUNK, :] * LOG2E - m)
            elif start >= tokens:
                g = (start - tokens) // CHUNK
                p = jnp.exp2(s_ref[slot, start:start + CHUNK, :] * LOG2E + (log_mult_pair[g:g + 1, :] - m))
            else:
                p = jnp.concatenate([jnp.exp2(s_ref[slot, start + r * RUN:start + (r + 1) * RUN, :] * LOG2E + (log_mult[r:r + 1, :] - m))
                                     for r in range(CLASSES)], axis=0)
            total = total + fold_rows(p, jnp.add)
            part = dot_nn(vt_ref[:, start:start + CHUNK], p.astype(BF16))
            acc = part if acc is None else acc + part
        l = jnp.sum(total, axis=0, keepdims=True)
        out = acc * (1.0 / l)
        lanes = (2 * pair + (0 if matched else 1)) * CHUNK
        ot_ref[0, :, lanes:lanes + CHUNK] = out.astype(BF16)
        if matched:
            st_ref[0, :, pair * 128:(pair + 1) * 128] = out[:, :128]
            lse_ref[0, :, pair * 128:(pair + 1) * 128] = jnp.broadcast_to((m + jnp.log2(l))[:, :128], (8, 128))

    tiles = [(matched, pair) for pair in range(n_pairs) for matched in (True, False)]
    tiles = [(matched, pair, n % 2) for n, (matched, pair) in enumerate(tiles)]
    m = scores(tiles[0])
    for tile, following in zip(tiles, tiles[1:] + [None]):
        m_following = None if following is None else scores(following)
        values(tile, m)
        m = m_following


def local_attention(flags, q, k, v, pair_k, pair_v, first_head, count, previous, after):
    num_heads, tokens, width = q.shape
    shapes = [jax.ShapeDtypeStruct((num_heads, width, tokens), BF16),
              jax.ShapeDtypeStruct((num_heads, width, tokens // 4), F32),
              jax.ShapeDtypeStruct((num_heads, 8, tokens // 4), F32),
              jax.ShapeDtypeStruct((num_heads, tokens // 4, width), BF16)]
    ins = (q, k, v, pair_k, pair_v)
    extra = tuple(previous) + tuple(after)
    return pl.pallas_call(
        lambda *refs: local_kernel(first_head, *refs),
        grid_spec=pltpu.PrefetchScalarGridSpec(
            num_scalar_prefetch=1,
            grid=(count,),
            in_specs=[head_spec(a.shape, first_head) for a in ins] + [pl.BlockSpec(memory_space=pl.ANY)] * len(extra),
            out_specs=[head_spec(s.shape, first_head) for s in shapes],
            scratch_shapes=[pltpu.VMEM((width, tokens + pair_k.shape[1]), BF16),
                            pltpu.VMEM((2, tokens + pair_k.shape[1], CHUNK), F32)],
        ),
        out_shape=shapes,
        input_output_aliases={len(ins) + 1 + n: n for n in range(len(previous))},
        compiler_params=params(),
        cost_estimate=pl.CostEstimate(flops=count * 5 * 10 ** 9, bytes_accessed=count * 10 ** 7, transcendentals=count * 4 * 10 ** 6),
        name="local_attention",
    )(flags, *ins, *extra)


def far_kernel(flag_ref, qa_ref, qb_ref, *refs):
    keys, values, outs = refs[:4], refs[4:8], refs[-4:]

    @pl.when(flag_ref[2] == 1)
    def _():
        turned = [jnp.transpose(v_ref[0]) for v_ref in values]
        for side, q_ref in enumerate((qa_ref, qb_ref)):
            scores = [dot_nt(k_ref[0], q_ref[0]) for k_ref in keys]
            m = fold_rows(scores[0], jnp.maximum)
            for s in scores[1:]:
                m = jnp.maximum(m, fold_rows(s, jnp.maximum))
            m = jnp.max(m, axis=0, keepdims=True) * LOG2E
            total = jnp.zeros((8, CHUNK), F32)
            acc = None
            for s, vt in zip(scores, turned):
                p = jnp.exp2(s * LOG2E - m)
                total = total + fold_rows(p, jnp.add)
                part = dot_nn(vt, p.astype(BF16))
                acc = part if acc is None else acc + part
            l = jnp.sum(total, axis=0, keepdims=True)
            outs[2 * side][0] = acc * (1.0 / l)
            outs[2 * side + 1][0] = jnp.broadcast_to(m + jnp.log2(l), (8, CHUNK))


def far_attention(flags, q_own, q_later, keys, values, after):
    num_heads, rows, width = q_own.shape
    shapes = [jax.ShapeDtypeStruct((num_heads, width, rows), F32), jax.ShapeDtypeStruct((num_heads, 8, rows), F32)] * 2
    ins = (q_own, q_later, *keys, *values)
    return pl.pallas_call(
        far_kernel,
        grid_spec=pltpu.PrefetchScalarGridSpec(
            num_scalar_prefetch=1,
            grid=(num_heads,),
            in_specs=[head_spec(a.shape) for a in ins] + [pl.BlockSpec(memory_space=pl.ANY)] * len(after),
            out_specs=[head_spec(s.shape) for s in shapes],
        ),
        out_shape=shapes,
        compiler_params=params(),
        cost_estimate=pl.CostEstimate(flops=5 * 10 ** 9, bytes_accessed=2 * 10 ** 7, transcendentals=4 * 10 ** 6),
        name="far_attention",
    )(flags, *ins, *after)


def final_kernel(num_heads, flag_ref, q_ref, ot_ref, st_ref, lse_ref, k0_ref, k1_ref, v0_ref, v1_ref,
                 fo0_ref, fl0_ref, fo1_ref, fl1_ref, wo_ref, y_ref, o_ref, merged_ref):
    step = pl.program_id(0)

    @pl.when(step < num_heads)
    def _():
        head = step
        lane = lax.broadcasted_iota(jnp.int32, (8, CHUNK), 1)
        first = (lane % 128) < 64

        def merge(with_quad):
            far_lse = jnp.where(flag_ref[2] == 1, fl0_ref[0], jnp.where(flag_ref[3] == 1, fl1_ref[0], -jnp.inf))
            for half in range(2):
                lanes = slice(half * CHUNK, (half + 1) * CHUNK)
                block = slice(half * 128, (half + 1) * 128)
                far = jnp.where(flag_ref[2] == 1, fo0_ref[0, :, block], jnp.where(flag_ref[3] == 1, fo1_ref[0, :, block], 0.0))
                far = jnp.concatenate([far, pltpu.roll(far, 64, 1)], axis=1)
                f_lse = far_lse[:, block]
                f_lse = jnp.where(first, jnp.concatenate([f_lse, pltpu.roll(f_lse, 64, 1)], axis=1), -jnp.inf)
                lse = lse_ref[0, :, lanes]
                m = jnp.maximum(lse, f_lse)
                scores = []
                if with_quad:
                    q = q_ref[0, lanes, :]
                    for k_ref in (k0_ref, k1_ref):
                        for g in range(2):
                            s = dot_nt(k_ref[0, g * CHUNK:(g + 1) * CHUNK, :], q) * LOG2E
                            if g == 0:
                                s = s + jnp.where(first, 1.0, 0.0)[:1, :]
                            scores.append(s)
                            m = jnp.maximum(m, fold_rows(s, jnp.maximum))
                m = jnp.max(m, axis=0, keepdims=True)
                own_weight = jnp.exp2(lse[:1, :] - m)
                far_weight = jnp.exp2(f_lse[:1, :] - m)
                out = st_ref[0, :, lanes] * own_weight + far * far_weight
                l = own_weight + far_weight
                total = jnp.zeros((8, CHUNK), F32)
                acc = None
                for n, s in enumerate(scores):
                    p = jnp.exp2(s - m)
                    total = total + fold_rows(p, jnp.add)
                    values = jnp.transpose((v0_ref, v1_ref)[n // 2][0, n % 2 * CHUNK:(n % 2 + 1) * CHUNK, :])
                    part = dot_nn(values, p.astype(BF16))
                    acc = part if acc is None else acc + part
                if with_quad:
                    out = out + acc
                    l = l + jnp.sum(total, axis=0, keepdims=True)
                merged_ref[:, lanes] = (out * (1.0 / l)).astype(BF16)

        @pl.when(flag_ref[1] == 1)
        def _():
            merge(True)

        @pl.when(flag_ref[1] == 0)
        def _():
            merge(False)

        token = lax.broadcasted_iota(jnp.int32, (2 * CHUNK, CHUNK), 0)
        column = lax.broadcasted_iota(jnp.int32, (2 * CHUNK, CHUNK), 1)
        places = [(token == lane_position(column, c)).astype(F32).astype(BF16) for c in (head, head ^ 1)]
        for pair in range(4):
            start = 2 * pair * CHUNK
            matched = jnp.concatenate([merged_ref[:, pair * 128:(pair + 1) * 128],
                                       ot_ref[0, :, start + 128:start + CHUNK]], axis=1)
            rows = dot_nt(places[0], matched) + dot_nt(places[1], ot_ref[0, :, start + CHUNK:start + 2 * CHUNK])
            columns = pl.ds(pl.multiple_of(head * CHUNK, CHUNK), CHUNK)
            o_ref[start:start + 2 * CHUNK, columns] = rows.astype(BF16)

    @pl.when(step >= num_heads)
    def _():
        y_ref[...] = dot_nn(o_ref[...], wo_ref[...]).astype(BF16)


def final_attention(flags, q, ot, st, lse, keys, values, far, w_out):
    num_heads, width, tokens = ot.shape
    d_model = w_out.shape[1]
    ins = (q, ot, st, lse, *keys, *values, *far)
    column = lambda h, flags: (0, jnp.maximum(h - num_heads, 0))
    return pl.pallas_call(
        lambda *refs: final_kernel(num_heads, *refs),
        grid_spec=pltpu.PrefetchScalarGridSpec(
            num_scalar_prefetch=1,
            grid=(num_heads + d_model // 256,),
            in_specs=[head_spec(a.shape, last=num_heads - 1) for a in ins] + [pl.BlockSpec((w_out.shape[0], 256), column)],
            out_specs=pl.BlockSpec((tokens, 256), column),
            scratch_shapes=[pltpu.VMEM((tokens, num_heads * width), BF16), pltpu.VMEM((width, tokens // 4), BF16)],
        ),
        out_shape=jax.ShapeDtypeStruct((tokens, d_model), BF16),
        compiler_params=params(),
        cost_estimate=pl.CostEstimate(flops=3 * 10 ** 10, bytes_accessed=6 * 10 ** 7, transcendentals=5 * 10 ** 6),
        name="final_attention",
    )(flags, *ins, w_out)


def solution(mesh):
    row_spec = P(('dp', 'seq'), None)
    pair_up = [(s, s + 1) for s in (0, 2, 4, 6)]
    next_chip = [(0, 2), (1, 3), (4, 6), (5, 7)]
    swap_upper = [(s, s ^ 1) for s in (2, 3, 6, 7)]
    from_first = [(0, 4), (1, 5)]
    from_second = [(2, 4), (3, 5)]
    swap_third = [(4, 5), (5, 4)]
    to_third = [(6, 4), (7, 5)]
    to_fourth = [(4, 6), (5, 7)]

    def send(array, pairs):
        return lax.ppermute(array, 'seq', pairs)

    def layer(hidden, w_query, w_key, w_value, w_out):
        _, d_model = hidden.shape
        num_heads, head_dim = w_query.shape[1:]
        index = lax.axis_index('seq')
        chip = index // 2
        flags = jnp.stack([index % 2, chip % 2, (chip == 2).astype(jnp.int32), (chip == 3).astype(jnp.int32)]).astype(jnp.int32)

        x = sort_by_class(hidden)

        def project(weight):
            return jnp.einsum('td,dhe->hte', x, weight, preferred_element_type=F32)

        def spread(packs):
            far_rows, quad_rows, pair_rows = packs
            first = send(far_rows, from_first)
            second = send(far_rows, from_second)
            quad = send(quad_rows, next_chip)
            pair = send(pair_rows, pair_up)
            swapped = send(first, swap_third), send(second, swap_third)
            return pair, (quad, send(quad, swap_upper)), (first, second, *swapped)

        k = project(w_key).astype(BF16)
        pair_k, quad_k, far_k = spread(pack(k, (1, 2, 4)))
        v = project(w_value).astype(BF16)
        pair_v, quad_v, far_v = spread(pack(v, (1, 2, 4)))
        q = (project(w_query) * head_dim ** -0.5).astype(BF16)
        q_far, = pack(q, (1,))
        q_later = send(q_far, to_third)

        early = 2
        state = local_attention(flags, q, k, v, pair_k, pair_v, 0, early, (), ())
        own_o, own_lse, later_o, later_lse = far_attention(flags, q_far, q_later, far_k, far_v, (state[2],))
        got_o, got_lse = send(later_o, to_fourth), send(later_lse, to_fourth)
        ot, st, lse, q_late = local_attention(flags, q, k, v, pair_k, pair_v, early, num_heads - early, state, (own_lse,))
        return final_attention(flags, q_late, ot, st, lse, quad_k, quad_v, (own_o, own_lse, got_o, got_lse),
                               w_out.reshape(num_heads * head_dim, d_model))

    return jax.shard_map(layer, mesh=mesh, in_specs=(row_spec, P(), P(), P(), P()), out_specs=row_spec, check_vma=False)
```

```python
import math
import jax
import jax.numpy as jnp
from jax import lax
from jax.experimental import pallas as pl
from jax.experimental.pallas import tpu as pltpu
from jax.sharding import PartitionSpec as P

CHUNK = 256
CLASSES = 8
RUN = CHUNK // CLASSES
LOG2E = math.log2(math.e)
F32 = jnp.float32
BF16 = jnp.bfloat16
VMEM_LIMIT = 60 * 1024 * 1024


def params():
    return pltpu.CompilerParams(vmem_limit_bytes=VMEM_LIMIT, dimension_semantics=("arbitrary",))


def dot_nt(a, b):
    return lax.dot_general(a, b, (((1,), (1,)), ((), ())), preferred_element_type=F32)


def dot_nn(a, b):
    return lax.dot_general(a, b, (((1,), (0,)), ((), ())), preferred_element_type=F32)


def class_of_group(head, group):
    return head ^ (0, 4, 2, 6)[group]


def run_rows(chunk, cls):
    return pl.ds(pl.multiple_of(chunk * CHUNK + cls * RUN, RUN), RUN)


def gather_tile(ref, pair, classes):
    return jnp.concatenate([ref[0, run_rows(2 * pair + b, cls), :] for cls in classes for b in range(2)], axis=0)


def lane_class(lane):
    group = lane // (2 * RUN)
    return (group % 2) * 4 + (group // 2) * 2


def lane_position(lane, first_class):
    return (lane // RUN) % 2 * CHUNK + lane % RUN * CLASSES + (lane_class(lane) ^ first_class)


def fold_rows(x, op):
    while x.shape[0] > 8:
        half = x.shape[0] // 2
        x = op(x[:half], x[half:])
    return x


def pack_kernel(n_groups, *refs):
    src_refs, out_refs = refs[:n_groups], refs[n_groups:]
    for group, src_ref in enumerate(src_refs):
        rows = src_ref.shape[1] * RUN
        block = src_ref[...].reshape(rows, src_ref.shape[-1])
        for out_ref in out_refs:
            if out_ref.shape[1] > group * rows:
                out_ref[0, group * rows:(group + 1) * rows, :] = block


def pack(src, group_counts):
    num_heads, tokens, width = src.shape
    n_chunks = tokens // CHUNK
    shapes = [(num_heads, tokens // CLASSES * count, width) for count in group_counts]
    n_groups = max(group_counts)
    runs = src.reshape(num_heads, n_chunks, CLASSES, RUN, width)

    def run_spec(group):
        return pl.BlockSpec((1, n_chunks, 1, RUN, width), lambda h: (h, 0, class_of_group(h, group), 0, 0))

    return pl.pallas_call(
        lambda *refs: pack_kernel(n_groups, *refs),
        grid=(num_heads,),
        out_shape=[jax.ShapeDtypeStruct(s, BF16) for s in shapes],
        in_specs=[run_spec(group) for group in range(n_groups)],
        out_specs=[pl.BlockSpec((1,) + s[1:], lambda h: (h, 0, 0)) for s in shapes],
        compiler_params=params(),
        cost_estimate=pl.CostEstimate(flops=10 ** 8, bytes_accessed=3 * src.size, transcendentals=0),
        name="pack",
    )(*[runs] * n_groups)


def sort_kernel(x_ref, y_ref, perm_ref):
    @pl.when(pl.program_id(0) == 0)
    def _():
        row = lax.broadcasted_iota(jnp.int32, (CHUNK, CHUNK), 0)
        col = lax.broadcasted_iota(jnp.int32, (CHUNK, CHUNK), 1)
        perm_ref[...] = (col == (row % RUN) * CLASSES + row // RUN).astype(F32).astype(BF16)

    y_ref[...] = dot_nn(perm_ref[...], x_ref[...]).astype(BF16)


def sort_by_class(x):
    tokens, width = x.shape
    spec = pl.BlockSpec((CHUNK, width), lambda i: (i, 0))
    return pl.pallas_call(
        sort_kernel,
        grid=(tokens // CHUNK,),
        out_shape=jax.ShapeDtypeStruct(x.shape, BF16),
        in_specs=[spec],
        out_specs=spec,
        scratch_shapes=[pltpu.VMEM((CHUNK, CHUNK), BF16)],
        compiler_params=params(),
        cost_estimate=pl.CostEstimate(flops=2 * 10 ** 9, bytes_accessed=4 * x.size, transcendentals=0),
        name="sort_by_class",
    )(x)


def head_spec(shape, first=0, last=None, flag=None):
    def index(h, flags):
        block = h + first if last is None else jnp.minimum(h, last)
        return (block if flag is None else block * flags[flag], 0, 0)

    return pl.BlockSpec((1,) + shape[1:], index)


def local_kernel(first_head, flag_ref, q_ref, k_ref, v_ref, pk_ref, pv_ref, *refs):
    ot_ref, st_ref, lse_ref, late_ref, vt_ref, s_ref = refs[-6:]
    head = pl.program_id(0) + first_head
    tokens = q_ref.shape[1]
    n_pairs = tokens // (2 * CHUNK)
    vt_ref[:, :tokens] = jnp.transpose(v_ref[0])
    vt_ref[:, tokens:] = jnp.transpose(pv_ref[0])

    lane = lax.broadcasted_iota(jnp.int32, (8, CHUNK), 1)
    row = lax.broadcasted_iota(jnp.int32, (8, CHUNK), 0)
    both = (row ^ head) | lane_class(lane)
    log_mult = jnp.where(both == 0, 2.0, jnp.where(both % 4 == 0, math.log2(3.0), jnp.where(both % 2 == 0, 1.0, 0.0)))
    both = lane_class(row * 2 * RUN) | lane_class(lane)
    log_mult_pair = jnp.where(both == 0, math.log2(3.0), jnp.where(both % 4 == 0, 1.0, 0.0))
    log_mult_pair = jnp.where(flag_ref[0] == 1, log_mult_pair, -jnp.inf)
    row_run = lax.broadcasted_iota(jnp.int32, (RUN, CHUNK), 0) * CLASSES
    lane_run = lax.broadcasted_iota(jnp.int32, (RUN, CHUNK), 1)

    def scores(tile):
        matched, pair, slot = tile
        first = head if matched else head ^ 1
        q = gather_tile(q_ref, pair, [class_of_group(first, g) for g in range(4)])
        if matched:
            late_ref[0, pair * 128:(pair + 1) * 128, :] = q[:128, :]
        limit = lane_position(lane_run, first) - row_run
        m = jnp.full((8, CHUNK), -jnp.inf, F32)
        for j in range(2 * pair + 2):
            s = dot_nt(k_ref[0, j * CHUNK:(j + 1) * CHUNK, :], q)
            for r in range(CLASSES):
                part = s[r * RUN:(r + 1) * RUN, :]
                if j >= 2 * pair:
                    part = jnp.where(limit >= (j - 2 * pair) * CHUNK + r, part, -jnp.inf)
                s_ref[slot, j * CHUNK + r * RUN:j * CHUNK + (r + 1) * RUN, :] = part
                m = jnp.maximum(m, fold_rows(part, jnp.maximum))
        if matched:
            m_pair = jnp.full((8, CHUNK), -jnp.inf, F32)
            for g in range(4):
                s = dot_nt(pk_ref[0, g * CHUNK:(g + 1) * CHUNK, :], q)
                s_ref[slot, tokens + g * CHUNK:tokens + (g + 1) * CHUNK, :] = s
                m_pair = jnp.maximum(m_pair, fold_rows(s, jnp.maximum))
            m = jnp.maximum(m, jnp.where(flag_ref[0] == 1, m_pair, -jnp.inf))
        return jnp.max(m, axis=0, keepdims=True) * LOG2E

    def values(tile, m):
        matched, pair, slot = tile
        starts = [j * CHUNK for j in range(2 * pair + 2)] + ([tokens + g * CHUNK for g in range(4)] if matched else [])
        total = jnp.zeros((8, CHUNK), F32)
        acc = None
        for start in starts:
            if not matched:
                p = jnp.exp2(s_ref[slot, start:start + CHUNK, :] * LOG2E - m)
            elif start >= tokens:
                g = (start - tokens) // CHUNK
                p = jnp.exp2(s_ref[slot, start:start + CHUNK, :] * LOG2E + (log_mult_pair[g:g + 1, :] - m))
            else:
                p = jnp.concatenate([jnp.exp2(s_ref[slot, start + r * RUN:start + (r + 1) * RUN, :] * LOG2E + (log_mult[r:r + 1, :] - m))
                                     for r in range(CLASSES)], axis=0)
            total = total + fold_rows(p, jnp.add)
            part = dot_nn(vt_ref[:, start:start + CHUNK], p.astype(BF16))
            acc = part if acc is None else acc + part
        l = jnp.sum(total, axis=0, keepdims=True)
        out = acc * (1.0 / l)
        lanes = (2 * pair + (0 if matched else 1)) * CHUNK
        ot_ref[0, :, lanes:lanes + CHUNK] = out.astype(BF16)
        if matched:
            st_ref[0, :, pair * 128:(pair + 1) * 128] = out[:, :128]
            lse_ref[0, :, pair * 128:(pair + 1) * 128] = jnp.broadcast_to((m + jnp.log2(l))[:, :128], (8, 128))

    tiles = [(matched, pair) for pair in range(n_pairs) for matched in (True, False)]
    tiles = [(matched, pair, n % 2) for n, (matched, pair) in enumerate(tiles)]
    m = scores(tiles[0])
    for tile, following in zip(tiles, tiles[1:] + [None]):
        m_following = None if following is None else scores(following)
        values(tile, m)
        m = m_following


def local_attention(flags, q, k, v, pair_k, pair_v, first_head, count, previous, after):
    num_heads, tokens, width = q.shape
    shapes = [jax.ShapeDtypeStruct((num_heads, width, tokens), BF16),
              jax.ShapeDtypeStruct((num_heads, width, tokens // 4), F32),
              jax.ShapeDtypeStruct((num_heads, 8, tokens // 4), F32),
              jax.ShapeDtypeStruct((num_heads, tokens // 4, width), BF16)]
    ins = (q, k, v, pair_k, pair_v)
    extra = tuple(previous) + tuple(after)
    return pl.pallas_call(
        lambda *refs: local_kernel(first_head, *refs),
        grid_spec=pltpu.PrefetchScalarGridSpec(
            num_scalar_prefetch=1,
            grid=(count,),
            in_specs=[head_spec(a.shape, first_head) for a in ins] + [pl.BlockSpec(memory_space=pl.ANY)] * len(extra),
            out_specs=[head_spec(s.shape, first_head) for s in shapes],
            scratch_shapes=[pltpu.VMEM((width, tokens + pair_k.shape[1]), BF16),
                            pltpu.VMEM((2, tokens + pair_k.shape[1], CHUNK), F32)],
        ),
        out_shape=shapes,
        input_output_aliases={len(ins) + 1 + n: n for n in range(len(previous))},
        compiler_params=params(),
        cost_estimate=pl.CostEstimate(flops=count * 5 * 10 ** 9, bytes_accessed=count * 10 ** 7, transcendentals=count * 4 * 10 ** 6),
        name="local_attention",
    )(flags, *ins, *extra)


def far_kernel(flag_ref, qa_ref, qb_ref, *refs):
    keys, values, outs = refs[:4], refs[4:8], refs[-4:]

    @pl.when(flag_ref[2] == 1)
    def _():
        turned = [jnp.transpose(v_ref[0]) for v_ref in values]
        for side, q_ref in enumerate((qa_ref, qb_ref)):
            scores = [dot_nt(k_ref[0], q_ref[0]) for k_ref in keys]
            m = fold_rows(scores[0], jnp.maximum)
            for s in scores[1:]:
                m = jnp.maximum(m, fold_rows(s, jnp.maximum))
            m = jnp.max(m, axis=0, keepdims=True) * LOG2E
            total = jnp.zeros((8, CHUNK), F32)
            acc = None
            for s, vt in zip(scores, turned):
                p = jnp.exp2(s * LOG2E - m)
                total = total + fold_rows(p, jnp.add)
                part = dot_nn(vt, p.astype(BF16))
                acc = part if acc is None else acc + part
            l = jnp.sum(total, axis=0, keepdims=True)
            outs[2 * side][0] = acc * (1.0 / l)
            outs[2 * side + 1][0] = jnp.broadcast_to(m + jnp.log2(l), (8, CHUNK))


def far_attention(flags, q_own, q_later, keys, values, after):
    num_heads, rows, width = q_own.shape
    shapes = [jax.ShapeDtypeStruct((num_heads, width, rows), F32), jax.ShapeDtypeStruct((num_heads, 8, rows), F32)] * 2
    ins = (q_own, q_later, *keys, *values)
    return pl.pallas_call(
        far_kernel,
        grid_spec=pltpu.PrefetchScalarGridSpec(
            num_scalar_prefetch=1,
            grid=(num_heads,),
            in_specs=[head_spec(a.shape, flag=2) for a in ins] + [pl.BlockSpec(memory_space=pl.ANY)] * len(after),
            out_specs=[head_spec(s.shape, flag=2) for s in shapes],
        ),
        out_shape=shapes,
        compiler_params=params(),
        cost_estimate=pl.CostEstimate(flops=5 * 10 ** 9, bytes_accessed=2 * 10 ** 7, transcendentals=4 * 10 ** 6),
        name="far_attention",
    )(flags, *ins, *after)


def final_kernel(num_heads, flag_ref, q_ref, ot_ref, st_ref, lse_ref, k0_ref, k1_ref, v0_ref, v1_ref,
                 fo0_ref, fl0_ref, fo1_ref, fl1_ref, wo_ref, y_ref, o_ref, merged_ref):
    step = pl.program_id(0)

    @pl.when(step < num_heads)
    def _():
        head = step
        lane = lax.broadcasted_iota(jnp.int32, (8, CHUNK), 1)
        first = (lane % 128) < 64

        def merge(with_quad):
            far_lse = jnp.where(flag_ref[2] == 1, fl0_ref[0], jnp.where(flag_ref[3] == 1, fl1_ref[0], -jnp.inf))
            for half in range(2):
                lanes = slice(half * CHUNK, (half + 1) * CHUNK)
                block = slice(half * 128, (half + 1) * 128)
                far = jnp.where(flag_ref[2] == 1, fo0_ref[0, :, block], jnp.where(flag_ref[3] == 1, fo1_ref[0, :, block], 0.0))
                far = jnp.concatenate([far, pltpu.roll(far, 64, 1)], axis=1)
                f_lse = far_lse[:, block]
                f_lse = jnp.where(first, jnp.concatenate([f_lse, pltpu.roll(f_lse, 64, 1)], axis=1), -jnp.inf)
                lse = lse_ref[0, :, lanes]
                m = jnp.maximum(lse, f_lse)
                scores = []
                if with_quad:
                    q = q_ref[0, lanes, :]
                    for k_ref in (k0_ref, k1_ref):
                        for g in range(2):
                            s = dot_nt(k_ref[0, g * CHUNK:(g + 1) * CHUNK, :], q) * LOG2E
                            if g == 0:
                                s = s + jnp.where(first, 1.0, 0.0)[:1, :]
                            scores.append(s)
                            m = jnp.maximum(m, fold_rows(s, jnp.maximum))
                m = jnp.max(m, axis=0, keepdims=True)
                own_weight = jnp.exp2(lse[:1, :] - m)
                far_weight = jnp.exp2(f_lse[:1, :] - m)
                out = st_ref[0, :, lanes] * own_weight + far * far_weight
                l = own_weight + far_weight
                total = jnp.zeros((8, CHUNK), F32)
                acc = None
                for n, s in enumerate(scores):
                    p = jnp.exp2(s - m)
                    total = total + fold_rows(p, jnp.add)
                    values = jnp.transpose((v0_ref, v1_ref)[n // 2][0, n % 2 * CHUNK:(n % 2 + 1) * CHUNK, :])
                    part = dot_nn(values, p.astype(BF16))
                    acc = part if acc is None else acc + part
                if with_quad:
                    out = out + acc
                    l = l + jnp.sum(total, axis=0, keepdims=True)
                merged_ref[:, lanes] = (out * (1.0 / l)).astype(BF16)

        @pl.when(flag_ref[1] == 1)
        def _():
            merge(True)

        @pl.when(flag_ref[1] == 0)
        def _():
            merge(False)

        token = lax.broadcasted_iota(jnp.int32, (2 * CHUNK, CHUNK), 0)
        column = lax.broadcasted_iota(jnp.int32, (2 * CHUNK, CHUNK), 1)
        places = [(token == lane_position(column, c)).astype(F32).astype(BF16) for c in (head, head ^ 1)]
        for pair in range(4):
            start = 2 * pair * CHUNK
            matched = jnp.concatenate([merged_ref[:, pair * 128:(pair + 1) * 128],
                                       ot_ref[0, :, start + 128:start + CHUNK]], axis=1)
            rows = dot_nt(places[0], matched) + dot_nt(places[1], ot_ref[0, :, start + CHUNK:start + 2 * CHUNK])
            columns = pl.ds(pl.multiple_of(head * CHUNK, CHUNK), CHUNK)
            o_ref[start:start + 2 * CHUNK, columns] = rows.astype(BF16)

    @pl.when(step >= num_heads)
    def _():
        y_ref[...] = dot_nn(o_ref[...], wo_ref[...]).astype(BF16)


def final_attention(flags, q, ot, st, lse, keys, values, far, w_out):
    num_heads, width, tokens = ot.shape
    d_model = w_out.shape[1]
    ins = (q, ot, st, lse, *keys, *values, *far)
    use = (1, None, None, None, 1, 1, 1, 1, 2, 2, 3, 3)
    column = lambda h, flags: (0, jnp.maximum(h - num_heads, 0))
    return pl.pallas_call(
        lambda *refs: final_kernel(num_heads, *refs),
        grid_spec=pltpu.PrefetchScalarGridSpec(
            num_scalar_prefetch=1,
            grid=(num_heads + d_model // 256,),
            in_specs=[head_spec(a.shape, last=num_heads - 1, flag=flag) for a, flag in zip(ins, use)] + [pl.BlockSpec((w_out.shape[0], 256), column)],
            out_specs=pl.BlockSpec((tokens, 256), column),
            scratch_shapes=[pltpu.VMEM((tokens, num_heads * width), BF16), pltpu.VMEM((width, tokens // 4), BF16)],
        ),
        out_shape=jax.ShapeDtypeStruct((tokens, d_model), BF16),
        compiler_params=params(),
        cost_estimate=pl.CostEstimate(flops=3 * 10 ** 10, bytes_accessed=6 * 10 ** 7, transcendentals=5 * 10 ** 6),
        name="final_attention",
    )(flags, *ins, w_out)


def solution(mesh):
    row_spec = P(('dp', 'seq'), None)
    swap = [(s, s ^ 1) for s in range(8)]
    next_chip = [(s, s ^ 2) for s in range(8)]
    from_first = [(0, 4), (4, 0), (1, 5), (5, 1), (2, 3), (3, 2), (6, 7), (7, 6)]
    from_second = [(2, 4), (4, 2), (3, 5), (5, 3), (0, 1), (1, 0), (6, 7), (7, 6)]
    to_third = [(6, 4), (7, 5)]
    to_fourth = [(4, 6), (6, 4), (5, 7), (7, 5), (0, 1), (1, 0), (2, 3), (3, 2)]

    def send(array, pairs):
        return lax.ppermute(array, 'seq', pairs)

    def layer(hidden, w_query, w_key, w_value, w_out):
        _, d_model = hidden.shape
        num_heads, head_dim = w_query.shape[1:]
        index = lax.axis_index('seq')
        chip = index // 2
        flags = jnp.stack([index % 2, chip % 2, (chip == 2).astype(jnp.int32), (chip == 3).astype(jnp.int32)]).astype(jnp.int32)

        x = sort_by_class(hidden)

        def project(weight):
            return jnp.einsum('td,dhe->hte', x, weight, preferred_element_type=F32)

        def spread(packs):
            far_rows, quad_rows, pair_rows = packs
            first = send(far_rows, from_first)
            second = send(far_rows, from_second)
            quad = send(quad_rows, next_chip)
            pair = send(pair_rows, swap)
            swapped = send(first, swap), send(second, swap)
            return pair, (quad, send(quad, swap)), (first, second, *swapped)

        k = project(w_key).astype(BF16)
        pair_k, quad_k, far_k = spread(pack(k, (1, 2, 4)))
        v = project(w_value).astype(BF16)
        pair_v, quad_v, far_v = spread(pack(v, (1, 2, 4)))
        q = (project(w_query) * head_dim ** -0.5).astype(BF16)
        q_far, = pack(q, (1,))
        q_later = send(q_far, to_third)

        early = 2
        state = local_attention(flags, q, k, v, pair_k, pair_v, 0, early, (), ())
        own_o, own_lse, later_o, later_lse = far_attention(flags, q_far, q_later, far_k, far_v, (state[2],))
        got_o, got_lse = send(later_o, to_fourth), send(later_lse, to_fourth)
        ot, st, lse, q_late = local_attention(flags, q, k, v, pair_k, pair_v, early, num_heads - early, state, (own_lse,))
        return final_attention(flags, q_late, ot, st, lse, quad_k, quad_v, (own_o, own_lse, got_o, got_lse),
                               w_out.reshape(num_heads * head_dim, d_model))

    return jax.shard_map(layer, mesh=mesh, in_specs=(row_spec, P(), P(), P(), P()), out_specs=row_spec, check_vma=False)
```

```python
import math
import jax
import jax.numpy as jnp
from jax import lax
from jax.experimental import pallas as pl
from jax.experimental.pallas import tpu as pltpu
from jax.sharding import PartitionSpec as P

CHUNK = 256
CLASSES = 8
RUN = CHUNK // CLASSES
LOG2E = math.log2(math.e)
F32 = jnp.float32
BF16 = jnp.bfloat16
VMEM_LIMIT = 60 * 1024 * 1024


def params():
    return pltpu.CompilerParams(vmem_limit_bytes=VMEM_LIMIT, dimension_semantics=("arbitrary",))


def dot_nt(a, b):
    return lax.dot_general(a, b, (((1,), (1,)), ((), ())), preferred_element_type=F32)


def dot_nn(a, b):
    return lax.dot_general(a, b, (((1,), (0,)), ((), ())), preferred_element_type=F32)


def class_of_group(head, group):
    return head ^ (0, 4, 2, 6)[group]


def run_rows(chunk, cls):
    return pl.ds(pl.multiple_of(chunk * CHUNK + cls * RUN, RUN), RUN)


def gather_tile(ref, pair, classes):
    return jnp.concatenate([ref[0, run_rows(2 * pair + b, cls), :] for cls in classes for b in range(2)], axis=0)


def lane_class(lane):
    group = lane // (2 * RUN)
    return (group % 2) * 4 + (group // 2) * 2


def lane_position(lane, first_class):
    return (lane // RUN) % 2 * CHUNK + lane % RUN * CLASSES + (lane_class(lane) ^ first_class)


def fold_rows(x, op):
    while x.shape[0] > 8:
        half = x.shape[0] // 2
        x = op(x[:half], x[half:])
    return x


def pack_kernel(n_groups, *refs):
    src_refs, out_refs = refs[:n_groups], refs[n_groups:]
    for group, src_ref in enumerate(src_refs):
        rows = src_ref.shape[1] * RUN
        block = src_ref[...].reshape(rows, src_ref.shape[-1])
        for out_ref in out_refs:
            if out_ref.shape[1] > group * rows:
                out_ref[0, group * rows:(group + 1) * rows, :] = block


def pack(src, group_counts):
    num_heads, tokens, width = src.shape
    n_chunks = tokens // CHUNK
    shapes = [(num_heads, tokens // CLASSES * count, width) for count in group_counts]
    n_groups = max(group_counts)
    runs = src.reshape(num_heads, n_chunks, CLASSES, RUN, width)

    def run_spec(group):
        return pl.BlockSpec((1, n_chunks, 1, RUN, width), lambda h: (h, 0, class_of_group(h, group), 0, 0))

    return pl.pallas_call(
        lambda *refs: pack_kernel(n_groups, *refs),
        grid=(num_heads,),
        out_shape=[jax.ShapeDtypeStruct(s, BF16) for s in shapes],
        in_specs=[run_spec(group) for group in range(n_groups)],
        out_specs=[pl.BlockSpec((1,) + s[1:], lambda h: (h, 0, 0)) for s in shapes],
        compiler_params=params(),
        cost_estimate=pl.CostEstimate(flops=10 ** 8, bytes_accessed=3 * src.size, transcendentals=0),
        name="pack",
    )(*[runs] * n_groups)


def sort_kernel(x_ref, y_ref, perm_ref):
    @pl.when(pl.program_id(0) == 0)
    def _():
        row = lax.broadcasted_iota(jnp.int32, (CHUNK, CHUNK), 0)
        col = lax.broadcasted_iota(jnp.int32, (CHUNK, CHUNK), 1)
        perm_ref[...] = (col == (row % RUN) * CLASSES + row // RUN).astype(F32).astype(BF16)

    y_ref[...] = dot_nn(perm_ref[...], x_ref[...]).astype(BF16)


def sort_by_class(x):
    tokens, width = x.shape
    spec = pl.BlockSpec((CHUNK, width), lambda i: (i, 0))
    return pl.pallas_call(
        sort_kernel,
        grid=(tokens // CHUNK,),
        out_shape=jax.ShapeDtypeStruct(x.shape, BF16),
        in_specs=[spec],
        out_specs=spec,
        scratch_shapes=[pltpu.VMEM((CHUNK, CHUNK), BF16)],
        compiler_params=params(),
        cost_estimate=pl.CostEstimate(flops=2 * 10 ** 9, bytes_accessed=4 * x.size, transcendentals=0),
        name="sort_by_class",
    )(x)


def head_spec(shape, first=0, last=None, flag=None):
    def index(h, flags):
        block = h + first if last is None else jnp.minimum(h, last)
        return (block if flag is None else block * flags[flag], 0, 0)

    return pl.BlockSpec((1,) + shape[1:], index)


def local_kernel(first_head, flag_ref, q_ref, k_ref, v_ref, pk_ref, pv_ref, *refs):
    ot_ref, st_ref, lse_ref, late_ref, vt_ref, s_ref = refs[-6:]
    head = pl.program_id(0) + first_head
    tokens = q_ref.shape[1]
    n_pairs = tokens // (2 * CHUNK)
    vt_ref[:, :tokens] = jnp.transpose(v_ref[0])
    vt_ref[:, tokens:] = jnp.transpose(pv_ref[0])

    lane = lax.broadcasted_iota(jnp.int32, (8, CHUNK), 1)
    row = lax.broadcasted_iota(jnp.int32, (8, CHUNK), 0)
    both = (row ^ head) | lane_class(lane)
    log_mult = jnp.where(both == 0, 2.0, jnp.where(both % 4 == 0, math.log2(3.0), jnp.where(both % 2 == 0, 1.0, 0.0)))
    both = lane_class(row * 2 * RUN) | lane_class(lane)
    log_mult_pair = jnp.where(both == 0, math.log2(3.0), jnp.where(both % 4 == 0, 1.0, 0.0))
    log_mult_pair = jnp.where(flag_ref[0] == 1, log_mult_pair, -jnp.inf)
    row_run = lax.broadcasted_iota(jnp.int32, (RUN, CHUNK), 0) * CLASSES
    lane_run = lax.broadcasted_iota(jnp.int32, (RUN, CHUNK), 1)

    def scores(tile):
        matched, pair, slot = tile
        first = head if matched else head ^ 1
        q = gather_tile(q_ref, pair, [class_of_group(first, g) for g in range(4)])
        if matched:
            late_ref[0, pair * 128:(pair + 1) * 128, :] = q[:128, :]
        limit = lane_position(lane_run, first) - row_run
        m = jnp.full((8, CHUNK), -jnp.inf, F32)
        for j in range(2 * pair + 2):
            s = dot_nt(k_ref[0, j * CHUNK:(j + 1) * CHUNK, :], q)
            for r in range(CLASSES):
                part = s[r * RUN:(r + 1) * RUN, :]
                if j >= 2 * pair:
                    part = jnp.where(limit >= (j - 2 * pair) * CHUNK + r, part, -jnp.inf)
                s_ref[slot, j * CHUNK + r * RUN:j * CHUNK + (r + 1) * RUN, :] = part
                m = jnp.maximum(m, fold_rows(part, jnp.maximum))
        if matched:
            m_pair = jnp.full((8, CHUNK), -jnp.inf, F32)
            for g in range(4):
                s = dot_nt(pk_ref[0, g * CHUNK:(g + 1) * CHUNK, :], q)
                s_ref[slot, tokens + g * CHUNK:tokens + (g + 1) * CHUNK, :] = s
                m_pair = jnp.maximum(m_pair, fold_rows(s, jnp.maximum))
            m = jnp.maximum(m, jnp.where(flag_ref[0] == 1, m_pair, -jnp.inf))
        return jnp.max(m, axis=0, keepdims=True) * LOG2E

    def values(tile, m):
        matched, pair, slot = tile
        starts = [j * CHUNK for j in range(2 * pair + 2)] + ([tokens + g * CHUNK for g in range(4)] if matched else [])
        total = jnp.zeros((8, CHUNK), F32)
        acc = None
        for start in starts:
            if not matched:
                p = jnp.exp2(s_ref[slot, start:start + CHUNK, :] * LOG2E - m)
            elif start >= tokens:
                g = (start - tokens) // CHUNK
                p = jnp.exp2(s_ref[slot, start:start + CHUNK, :] * LOG2E + (log_mult_pair[g:g + 1, :] - m))
            else:
                p = jnp.concatenate([jnp.exp2(s_ref[slot, start + r * RUN:start + (r + 1) * RUN, :] * LOG2E + (log_mult[r:r + 1, :] - m))
                                     for r in range(CLASSES)], axis=0)
            total = total + fold_rows(p, jnp.add)
            part = dot_nn(vt_ref[:, start:start + CHUNK], p.astype(BF16))
            acc = part if acc is None else acc + part
        l = jnp.sum(total, axis=0, keepdims=True)
        out = acc * (1.0 / l)
        lanes = (2 * pair + (0 if matched else 1)) * CHUNK
        ot_ref[0, :, lanes:lanes + CHUNK] = out.astype(BF16)
        if matched:
            st_ref[0, :, pair * 128:(pair + 1) * 128] = out[:, :128]
            lse_ref[0, :, pair * 128:(pair + 1) * 128] = jnp.broadcast_to((m + jnp.log2(l))[:, :128], (8, 128))

    tiles = [(matched, pair) for pair in range(n_pairs) for matched in (True, False)]
    tiles = [(matched, pair, n % 2) for n, (matched, pair) in enumerate(tiles)]
    m = scores(tiles[0])
    for tile, following in zip(tiles, tiles[1:] + [None]):
        m_following = None if following is None else scores(following)
        values(tile, m)
        m = m_following


def local_attention(flags, q, k, v, pair_k, pair_v, first_head, count, previous, after):
    num_heads, tokens, width = q.shape
    shapes = [jax.ShapeDtypeStruct((num_heads, width, tokens), BF16),
              jax.ShapeDtypeStruct((num_heads, width, tokens // 4), F32),
              jax.ShapeDtypeStruct((num_heads, 8, tokens // 4), F32),
              jax.ShapeDtypeStruct((num_heads, tokens // 4, width), BF16)]
    ins = (q, k, v, pair_k, pair_v)
    extra = tuple(previous) + tuple(after)
    return pl.pallas_call(
        lambda *refs: local_kernel(first_head, *refs),
        grid_spec=pltpu.PrefetchScalarGridSpec(
            num_scalar_prefetch=1,
            grid=(count,),
            in_specs=[head_spec(a.shape, first_head) for a in ins] + [pl.BlockSpec(memory_space=pl.ANY)] * len(extra),
            out_specs=[head_spec(s.shape, first_head) for s in shapes],
            scratch_shapes=[pltpu.VMEM((width, tokens + pair_k.shape[1]), BF16),
                            pltpu.VMEM((2, tokens + pair_k.shape[1], CHUNK), F32)],
        ),
        out_shape=shapes,
        input_output_aliases={len(ins) + 1 + n: n for n in range(len(previous))},
        compiler_params=params(),
        cost_estimate=pl.CostEstimate(flops=count * 5 * 10 ** 9, bytes_accessed=count * 10 ** 7, transcendentals=count * 4 * 10 ** 6),
        name="local_attention",
    )(flags, *ins, *extra)


def far_kernel(flag_ref, qa_ref, qb_ref, *refs):
    keys, values, outs = refs[:4], refs[4:8], refs[-4:]

    @pl.when(flag_ref[2] == 1)
    def _():
        turned = [jnp.transpose(v_ref[0]) for v_ref in values]
        for side, q_ref in enumerate((qa_ref, qb_ref)):
            scores = [dot_nt(k_ref[0], q_ref[0]) for k_ref in keys]
            m = fold_rows(scores[0], jnp.maximum)
            for s in scores[1:]:
                m = jnp.maximum(m, fold_rows(s, jnp.maximum))
            m = jnp.max(m, axis=0, keepdims=True) * LOG2E
            total = jnp.zeros((8, CHUNK), F32)
            acc = None
            for s, vt in zip(scores, turned):
                p = jnp.exp2(s * LOG2E - m)
                total = total + fold_rows(p, jnp.add)
                part = dot_nn(vt, p.astype(BF16))
                acc = part if acc is None else acc + part
            l = jnp.sum(total, axis=0, keepdims=True)
            outs[2 * side][0] = acc * (1.0 / l)
            outs[2 * side + 1][0] = jnp.broadcast_to(m + jnp.log2(l), (8, CHUNK))


def far_attention(flags, q_own, q_later, keys, values, after):
    num_heads, rows, width = q_own.shape
    shapes = [jax.ShapeDtypeStruct((num_heads, width, rows), F32), jax.ShapeDtypeStruct((num_heads, 8, rows), F32)] * 2
    ins = (q_own, q_later, *keys, *values)
    return pl.pallas_call(
        far_kernel,
        grid_spec=pltpu.PrefetchScalarGridSpec(
            num_scalar_prefetch=1,
            grid=(num_heads,),
            in_specs=[head_spec(a.shape, flag=2) for a in ins] + [pl.BlockSpec(memory_space=pl.ANY)] * len(after),
            out_specs=[head_spec(s.shape, flag=2) for s in shapes],
        ),
        out_shape=shapes,
        compiler_params=params(),
        cost_estimate=pl.CostEstimate(flops=5 * 10 ** 9, bytes_accessed=2 * 10 ** 7, transcendentals=4 * 10 ** 6),
        name="far_attention",
    )(flags, *ins, *after)


def final_kernel(num_heads, flag_ref, q_ref, ot_ref, st_ref, lse_ref, k0_ref, k1_ref, v0_ref, v1_ref,
                 fo0_ref, fl0_ref, fo1_ref, fl1_ref, wo_ref, y_ref, o_ref, merged_ref):
    step = pl.program_id(0)

    @pl.when(step < num_heads)
    def _():
        head = step
        lane = lax.broadcasted_iota(jnp.int32, (8, CHUNK), 1)
        first = (lane % 128) < 64

        def merge(with_quad):
            far_lse = jnp.where(flag_ref[2] == 1, fl0_ref[0], jnp.where(flag_ref[3] == 1, fl1_ref[0], -jnp.inf))
            for half in range(2):
                lanes = slice(half * CHUNK, (half + 1) * CHUNK)
                block = slice(half * 128, (half + 1) * 128)
                far = jnp.where(flag_ref[2] == 1, fo0_ref[0, :, block], jnp.where(flag_ref[3] == 1, fo1_ref[0, :, block], 0.0))
                far = jnp.concatenate([far, pltpu.roll(far, 64, 1)], axis=1)
                f_lse = far_lse[:, block]
                f_lse = jnp.where(first, jnp.concatenate([f_lse, pltpu.roll(f_lse, 64, 1)], axis=1), -jnp.inf)
                lse = lse_ref[0, :, lanes]
                m = jnp.maximum(lse, f_lse)
                scores = []
                if with_quad:
                    q = q_ref[0, lanes, :]
                    for k_ref in (k0_ref, k1_ref):
                        for g in range(2):
                            s = dot_nt(k_ref[0, g * CHUNK:(g + 1) * CHUNK, :], q) * LOG2E
                            if g == 0:
                                s = s + jnp.where(first, 1.0, 0.0)[:1, :]
                            scores.append(s)
                            m = jnp.maximum(m, fold_rows(s, jnp.maximum))
                m = jnp.max(m, axis=0, keepdims=True)
                own_weight = jnp.exp2(lse[:1, :] - m)
                far_weight = jnp.exp2(f_lse[:1, :] - m)
                out = st_ref[0, :, lanes] * own_weight + far * far_weight
                l = own_weight + far_weight
                total = jnp.zeros((8, CHUNK), F32)
                acc = None
                for n, s in enumerate(scores):
                    p = jnp.exp2(s - m)
                    total = total + fold_rows(p, jnp.add)
                    values = jnp.transpose((v0_ref, v1_ref)[n // 2][0, n % 2 * CHUNK:(n % 2 + 1) * CHUNK, :])
                    part = dot_nn(values, p.astype(BF16))
                    acc = part if acc is None else acc + part
                if with_quad:
                    out = out + acc
                    l = l + jnp.sum(total, axis=0, keepdims=True)
                merged_ref[:, lanes] = (out * (1.0 / l)).astype(BF16)

        @pl.when(flag_ref[1] == 1)
        def _():
            merge(True)

        @pl.when(flag_ref[1] == 0)
        def _():
            merge(False)

        token = lax.broadcasted_iota(jnp.int32, (2 * CHUNK, CHUNK), 0)
        column = lax.broadcasted_iota(jnp.int32, (2 * CHUNK, CHUNK), 1)
        places = [(token == lane_position(column, c)).astype(F32).astype(BF16) for c in (head, head ^ 1)]
        for pair in range(4):
            start = 2 * pair * CHUNK
            matched = jnp.concatenate([merged_ref[:, pair * 128:(pair + 1) * 128],
                                       ot_ref[0, :, start + 128:start + CHUNK]], axis=1)
            rows = dot_nt(places[0], matched) + dot_nt(places[1], ot_ref[0, :, start + CHUNK:start + 2 * CHUNK])
            columns = pl.ds(pl.multiple_of(head * CHUNK, CHUNK), CHUNK)
            o_ref[start:start + 2 * CHUNK, columns] = rows.astype(BF16)

    @pl.when(step >= num_heads)
    def _():
        y_ref[...] = dot_nn(o_ref[...], wo_ref[...]).astype(BF16)


def final_attention(flags, q, ot, st, lse, keys, values, far, w_out):
    num_heads, width, tokens = ot.shape
    d_model = w_out.shape[1]
    ins = (q, ot, st, lse, *keys, *values, *far)
    use = (1, None, None, None, 1, 1, 1, 1, 2, 2, 3, 3)
    column = lambda h, flags: (0, jnp.maximum(h - num_heads, 0))
    return pl.pallas_call(
        lambda *refs: final_kernel(num_heads, *refs),
        grid_spec=pltpu.PrefetchScalarGridSpec(
            num_scalar_prefetch=1,
            grid=(num_heads + d_model // 256,),
            in_specs=[head_spec(a.shape, last=num_heads - 1, flag=flag) for a, flag in zip(ins, use)] + [pl.BlockSpec((w_out.shape[0], 256), column)],
            out_specs=pl.BlockSpec((tokens, 256), column),
            scratch_shapes=[pltpu.VMEM((tokens, num_heads * width), BF16), pltpu.VMEM((width, tokens // 4), BF16)],
        ),
        out_shape=jax.ShapeDtypeStruct((tokens, d_model), BF16),
        compiler_params=params(),
        cost_estimate=pl.CostEstimate(flops=3 * 10 ** 10, bytes_accessed=6 * 10 ** 7, transcendentals=5 * 10 ** 6),
        name="final_attention",
    )(flags, *ins, w_out)


def solution(mesh):
    row_spec = P(('dp', 'seq'), None)
    swap = [(s, s ^ 1) for s in range(8)]
    next_chip = [(0, 2), (1, 3), (4, 6), (5, 7)]
    from_first = [(0, 4), (1, 5), (2, 3), (3, 2), (6, 7), (7, 6)]
    from_second = [(2, 4), (3, 5), (0, 1), (1, 0), (6, 7), (7, 6)]
    to_third = [(6, 4), (7, 5)]
    to_fourth = [(4, 6), (5, 7), (0, 1), (1, 0), (2, 3), (3, 2)]

    def send(array, pairs):
        return lax.ppermute(array, 'seq', pairs)

    def layer(hidden, w_query, w_key, w_value, w_out):
        _, d_model = hidden.shape
        num_heads, head_dim = w_query.shape[1:]
        index = lax.axis_index('seq')
        chip = index // 2
        flags = jnp.stack([index % 2, chip % 2, (chip == 2).astype(jnp.int32), (chip == 3).astype(jnp.int32)]).astype(jnp.int32)

        x = sort_by_class(hidden)

        def project(weight):
            return jnp.einsum('td,dhe->hte', x, weight, preferred_element_type=F32)

        def spread(packs):
            far_rows, quad_rows, pair_rows = packs
            first = send(far_rows, from_first)
            second = send(far_rows, from_second)
            quad = send(quad_rows, next_chip)
            pair = send(pair_rows, swap)
            swapped = send(first, swap), send(second, swap)
            return pair, (quad, send(quad, swap)), (first, second, *swapped)

        k = project(w_key).astype(BF16)
        pair_k, quad_k, far_k = spread(pack(k, (1, 2, 4)))
        v = project(w_value).astype(BF16)
        pair_v, quad_v, far_v = spread(pack(v, (1, 2, 4)))
        q = (project(w_query) * head_dim ** -0.5).astype(BF16)
        q_far, = pack(q, (1,))
        q_later = send(q_far, to_third)

        early = 2
        state = local_attention(flags, q, k, v, pair_k, pair_v, 0, early, (), ())
        own_o, own_lse, later_o, later_lse = far_attention(flags, q_far, q_later, far_k, far_v, (state[2],))
        got_o, got_lse = send(later_o, to_fourth), send(later_lse, to_fourth)
        ot, st, lse, q_late = local_attention(flags, q, k, v, pair_k, pair_v, early, num_heads - early, state, (own_lse,))
        return final_attention(flags, q_late, ot, st, lse, quad_k, quad_v, (own_o, own_lse, got_o, got_lse),
                               w_out.reshape(num_heads * head_dim, d_model))

    return jax.shard_map(layer, mesh=mesh, in_specs=(row_spec, P(), P(), P(), P()), out_specs=row_spec, check_vma=False)
```

```python
import math
import jax
import jax.numpy as jnp
from jax import lax
from jax.experimental import pallas as pl
from jax.experimental.pallas import tpu as pltpu
from jax.sharding import PartitionSpec as P

CHUNK = 256
CLASSES = 8
RUN = CHUNK // CLASSES
LOG2E = math.log2(math.e)
F32 = jnp.float32
BF16 = jnp.bfloat16
VMEM_LIMIT = 60 * 1024 * 1024


def params():
    return pltpu.CompilerParams(vmem_limit_bytes=VMEM_LIMIT, dimension_semantics=("arbitrary",))


def dot_nt(a, b):
    return lax.dot_general(a, b, (((1,), (1,)), ((), ())), preferred_element_type=F32)


def dot_nn(a, b):
    return lax.dot_general(a, b, (((1,), (0,)), ((), ())), preferred_element_type=F32)


def class_of_group(head, group):
    return head ^ (0, 4, 2, 6)[group]


def run_rows(chunk, cls):
    return pl.ds(pl.multiple_of(chunk * CHUNK + cls * RUN, RUN), RUN)


def gather_tile(ref, pair, classes):
    return jnp.concatenate([ref[0, run_rows(2 * pair + b, cls), :] for cls in classes for b in range(2)], axis=0)


def lane_class(lane):
    group = lane // (2 * RUN)
    return (group % 2) * 4 + (group // 2) * 2


def lane_position(lane, first_class):
    return (lane // RUN) % 2 * CHUNK + lane % RUN * CLASSES + (lane_class(lane) ^ first_class)


def fold_rows(x, op):
    while x.shape[0] > 8:
        half = x.shape[0] // 2
        x = op(x[:half], x[half:])
    return x


def pack_kernel(n_groups, *refs):
    src_refs, out_refs = refs[:n_groups], refs[n_groups:]
    for group, src_ref in enumerate(src_refs):
        rows = src_ref.shape[1] * RUN
        block = src_ref[...].reshape(rows, src_ref.shape[-1])
        for out_ref in out_refs:
            if out_ref.shape[1] > group * rows:
                out_ref[0, group * rows:(group + 1) * rows, :] = block


def pack(src, group_counts):
    num_heads, tokens, width = src.shape
    n_chunks = tokens // CHUNK
    shapes = [(num_heads, tokens // CLASSES * count, width) for count in group_counts]
    n_groups = max(group_counts)
    runs = src.reshape(num_heads, n_chunks, CLASSES, RUN, width)

    def run_spec(group):
        return pl.BlockSpec((1, n_chunks, 1, RUN, width), lambda h: (h, 0, class_of_group(h, group), 0, 0))

    return pl.pallas_call(
        lambda *refs: pack_kernel(n_groups, *refs),
        grid=(num_heads,),
        out_shape=[jax.ShapeDtypeStruct(s, BF16) for s in shapes],
        in_specs=[run_spec(group) for group in range(n_groups)],
        out_specs=[pl.BlockSpec((1,) + s[1:], lambda h: (h, 0, 0)) for s in shapes],
        compiler_params=params(),
        cost_estimate=pl.CostEstimate(flops=10 ** 8, bytes_accessed=3 * src.size, transcendentals=0),
        name="pack",
    )(*[runs] * n_groups)


def head_spec(shape, first=0, last=None, flag=None):
    def index(h, flags):
        block = h + first if last is None else jnp.minimum(h, last)
        return (block if flag is None else block * flags[flag], 0, 0)

    return pl.BlockSpec((1,) + shape[1:], index)


def local_kernel(first_head, flag_ref, q_ref, k_ref, v_ref, pk_ref, pv_ref, *refs):
    ot_ref, st_ref, lse_ref, late_ref, vt_ref, s_ref = refs[-6:]
    head = pl.program_id(0) + first_head
    tokens = q_ref.shape[1]
    n_pairs = tokens // (2 * CHUNK)
    vt_ref[:, :tokens] = jnp.transpose(v_ref[0])
    vt_ref[:, tokens:] = jnp.transpose(pv_ref[0])

    lane = lax.broadcasted_iota(jnp.int32, (8, CHUNK), 1)
    row = lax.broadcasted_iota(jnp.int32, (8, CHUNK), 0)
    both = (row ^ head) | lane_class(lane)
    log_mult = jnp.where(both == 0, 2.0, jnp.where(both % 4 == 0, math.log2(3.0), jnp.where(both % 2 == 0, 1.0, 0.0)))
    both = lane_class(row * 2 * RUN) | lane_class(lane)
    log_mult_pair = jnp.where(both == 0, math.log2(3.0), jnp.where(both % 4 == 0, 1.0, 0.0))
    log_mult_pair = jnp.where(flag_ref[0] == 1, log_mult_pair, -jnp.inf)
    row_run = lax.broadcasted_iota(jnp.int32, (RUN, CHUNK), 0) * CLASSES
    lane_run = lax.broadcasted_iota(jnp.int32, (RUN, CHUNK), 1)

    def scores(tile):
        matched, pair, slot = tile
        first = head if matched else head ^ 1
        q = gather_tile(q_ref, pair, [class_of_group(first, g) for g in range(4)])
        if matched:
            late_ref[0, pair * 128:(pair + 1) * 128, :] = q[:128, :]
        limit = lane_position(lane_run, first) - row_run
        m = jnp.full((8, CHUNK), -jnp.inf, F32)
        for j in range(2 * pair + 2):
            s = dot_nt(k_ref[0, j * CHUNK:(j + 1) * CHUNK, :], q)
            for r in range(CLASSES):
                part = s[r * RUN:(r + 1) * RUN, :]
                if j >= 2 * pair:
                    part = jnp.where(limit >= (j - 2 * pair) * CHUNK + r, part, -jnp.inf)
                s_ref[slot, j * CHUNK + r * RUN:j * CHUNK + (r + 1) * RUN, :] = part
                m = jnp.maximum(m, fold_rows(part, jnp.maximum))
        if matched:
            m_pair = jnp.full((8, CHUNK), -jnp.inf, F32)
            for g in range(4):
                s = dot_nt(pk_ref[0, g * CHUNK:(g + 1) * CHUNK, :], q)
                s_ref[slot, tokens + g * CHUNK:tokens + (g + 1) * CHUNK, :] = s
                m_pair = jnp.maximum(m_pair, fold_rows(s, jnp.maximum))
            m = jnp.maximum(m, jnp.where(flag_ref[0] == 1, m_pair, -jnp.inf))
        return jnp.max(m, axis=0, keepdims=True) * LOG2E

    def values(tile, m):
        matched, pair, slot = tile
        starts = [j * CHUNK for j in range(2 * pair + 2)] + ([tokens + g * CHUNK for g in range(4)] if matched else [])
        total = jnp.zeros((8, CHUNK), F32)
        acc = None
        for start in starts:
            if not matched:
                p = jnp.exp2(s_ref[slot, start:start + CHUNK, :] * LOG2E - m)
            elif start >= tokens:
                g = (start - tokens) // CHUNK
                p = jnp.exp2(s_ref[slot, start:start + CHUNK, :] * LOG2E + (log_mult_pair[g:g + 1, :] - m))
            else:
                p = jnp.concatenate([jnp.exp2(s_ref[slot, start + r * RUN:start + (r + 1) * RUN, :] * LOG2E + (log_mult[r:r + 1, :] - m))
                                     for r in range(CLASSES)], axis=0)
            total = total + fold_rows(p, jnp.add)
            part = dot_nn(vt_ref[:, start:start + CHUNK], p.astype(BF16))
            acc = part if acc is None else acc + part
        l = jnp.sum(total, axis=0, keepdims=True)
        out = acc * (1.0 / l)
        lanes = (2 * pair + (0 if matched else 1)) * CHUNK
        ot_ref[0, :, lanes:lanes + CHUNK] = out.astype(BF16)
        if matched:
            st_ref[0, :, pair * 128:(pair + 1) * 128] = out[:, :128]
            lse_ref[0, :, pair * 128:(pair + 1) * 128] = jnp.broadcast_to((m + jnp.log2(l))[:, :128], (8, 128))

    tiles = [(matched, pair) for pair in range(n_pairs) for matched in (True, False)]
    tiles = [(matched, pair, n % 2) for n, (matched, pair) in enumerate(tiles)]
    m = scores(tiles[0])
    for tile, following in zip(tiles, tiles[1:] + [None]):
        m_following = None if following is None else scores(following)
        values(tile, m)
        m = m_following


def local_attention(flags, q, k, v, pair_k, pair_v, first_head, count, previous, after):
    num_heads, tokens, width = q.shape
    shapes = [jax.ShapeDtypeStruct((num_heads, width, tokens), BF16),
              jax.ShapeDtypeStruct((num_heads, width, tokens // 4), F32),
              jax.ShapeDtypeStruct((num_heads, 8, tokens // 4), F32),
              jax.ShapeDtypeStruct((num_heads, tokens // 4, width), BF16)]
    ins = (q, k, v, pair_k, pair_v)
    extra = tuple(previous) + tuple(after)
    return pl.pallas_call(
        lambda *refs: local_kernel(first_head, *refs),
        grid_spec=pltpu.PrefetchScalarGridSpec(
            num_scalar_prefetch=1,
            grid=(count,),
            in_specs=[head_spec(a.shape, first_head) for a in ins] + [pl.BlockSpec(memory_space=pl.ANY)] * len(extra),
            out_specs=[head_spec(s.shape, first_head) for s in shapes],
            scratch_shapes=[pltpu.VMEM((width, tokens + pair_k.shape[1]), BF16),
                            pltpu.VMEM((2, tokens + pair_k.shape[1], CHUNK), F32)],
        ),
        out_shape=shapes,
        input_output_aliases={len(ins) + 1 + n: n for n in range(len(previous))},
        compiler_params=params(),
        cost_estimate=pl.CostEstimate(flops=count * 5 * 10 ** 9, bytes_accessed=count * 10 ** 7, transcendentals=count * 4 * 10 ** 6),
        name="local_attention",
    )(flags, *ins, *extra)


def far_kernel(flag_ref, qa_ref, qb_ref, *refs):
    keys, values, outs = refs[:4], refs[4:8], refs[-4:]

    @pl.when(flag_ref[2] == 1)
    def _():
        turned = [jnp.transpose(v_ref[0]) for v_ref in values]
        for side, q_ref in enumerate((qa_ref, qb_ref)):
            scores = [dot_nt(k_ref[0], q_ref[0]) for k_ref in keys]
            m = fold_rows(scores[0], jnp.maximum)
            for s in scores[1:]:
                m = jnp.maximum(m, fold_rows(s, jnp.maximum))
            m = jnp.max(m, axis=0, keepdims=True) * LOG2E
            total = jnp.zeros((8, CHUNK), F32)
            acc = None
            for s, vt in zip(scores, turned):
                p = jnp.exp2(s * LOG2E - m)
                total = total + fold_rows(p, jnp.add)
                part = dot_nn(vt, p.astype(BF16))
                acc = part if acc is None else acc + part
            l = jnp.sum(total, axis=0, keepdims=True)
            outs[2 * side][0] = acc * (1.0 / l)
            outs[2 * side + 1][0] = jnp.broadcast_to(m + jnp.log2(l), (8, CHUNK))


def far_attention(flags, q_own, q_later, keys, values, after):
    num_heads, rows, width = q_own.shape
    shapes = [jax.ShapeDtypeStruct((num_heads, width, rows), F32), jax.ShapeDtypeStruct((num_heads, 8, rows), F32)] * 2
    ins = (q_own, q_later, *keys, *values)
    return pl.pallas_call(
        far_kernel,
        grid_spec=pltpu.PrefetchScalarGridSpec(
            num_scalar_prefetch=1,
            grid=(num_heads,),
            in_specs=[head_spec(a.shape, flag=2) for a in ins] + [pl.BlockSpec(memory_space=pl.ANY)] * len(after),
            out_specs=[head_spec(s.shape, flag=2) for s in shapes],
        ),
        out_shape=shapes,
        compiler_params=params(),
        cost_estimate=pl.CostEstimate(flops=5 * 10 ** 9, bytes_accessed=2 * 10 ** 7, transcendentals=4 * 10 ** 6),
        name="far_attention",
    )(flags, *ins, *after)


def final_kernel(num_heads, flag_ref, q_ref, ot_ref, st_ref, lse_ref, k0_ref, k1_ref, v0_ref, v1_ref,
                 fo0_ref, fl0_ref, fo1_ref, fl1_ref, wo_ref, y_ref, o_ref, merged_ref):
    step = pl.program_id(0)

    @pl.when(step < num_heads)
    def _():
        head = step
        lane = lax.broadcasted_iota(jnp.int32, (8, CHUNK), 1)
        first = (lane % 128) < 64

        def merge(with_quad):
            far_lse = jnp.where(flag_ref[2] == 1, fl0_ref[0], jnp.where(flag_ref[3] == 1, fl1_ref[0], -jnp.inf))
            for half in range(2):
                lanes = slice(half * CHUNK, (half + 1) * CHUNK)
                block = slice(half * 128, (half + 1) * 128)
                far = jnp.where(flag_ref[2] == 1, fo0_ref[0, :, block], jnp.where(flag_ref[3] == 1, fo1_ref[0, :, block], 0.0))
                far = jnp.concatenate([far, pltpu.roll(far, 64, 1)], axis=1)
                f_lse = far_lse[:, block]
                f_lse = jnp.where(first, jnp.concatenate([f_lse, pltpu.roll(f_lse, 64, 1)], axis=1), -jnp.inf)
                lse = lse_ref[0, :, lanes]
                m = jnp.maximum(lse, f_lse)
                scores = []
                if with_quad:
                    q = q_ref[0, lanes, :]
                    for k_ref in (k0_ref, k1_ref):
                        for g in range(2):
                            s = dot_nt(k_ref[0, g * CHUNK:(g + 1) * CHUNK, :], q) * LOG2E
                            if g == 0:
                                s = s + jnp.where(first, 1.0, 0.0)[:1, :]
                            scores.append(s)
                            m = jnp.maximum(m, fold_rows(s, jnp.maximum))
                m = jnp.max(m, axis=0, keepdims=True)
                own_weight = jnp.exp2(lse[:1, :] - m)
                far_weight = jnp.exp2(f_lse[:1, :] - m)
                out = st_ref[0, :, lanes] * own_weight + far * far_weight
                l = own_weight + far_weight
                total = jnp.zeros((8, CHUNK), F32)
                acc = None
                for n, s in enumerate(scores):
                    p = jnp.exp2(s - m)
                    total = total + fold_rows(p, jnp.add)
                    values = jnp.transpose((v0_ref, v1_ref)[n // 2][0, n % 2 * CHUNK:(n % 2 + 1) * CHUNK, :])
                    part = dot_nn(values, p.astype(BF16))
                    acc = part if acc is None else acc + part
                if with_quad:
                    out = out + acc
                    l = l + jnp.sum(total, axis=0, keepdims=True)
                merged_ref[:, lanes] = (out * (1.0 / l)).astype(BF16)

        @pl.when(flag_ref[1] == 1)
        def _():
            merge(True)

        @pl.when(flag_ref[1] == 0)
        def _():
            merge(False)

        token = lax.broadcasted_iota(jnp.int32, (2 * CHUNK, CHUNK), 0)
        column = lax.broadcasted_iota(jnp.int32, (2 * CHUNK, CHUNK), 1)
        places = [(token == lane_position(column, c)).astype(F32).astype(BF16) for c in (head, head ^ 1)]
        for pair in range(4):
            start = 2 * pair * CHUNK
            matched = jnp.concatenate([merged_ref[:, pair * 128:(pair + 1) * 128],
                                       ot_ref[0, :, start + 128:start + CHUNK]], axis=1)
            rows = dot_nt(places[0], matched) + dot_nt(places[1], ot_ref[0, :, start + CHUNK:start + 2 * CHUNK])
            columns = pl.ds(pl.multiple_of(head * CHUNK, CHUNK), CHUNK)
            o_ref[start:start + 2 * CHUNK, columns] = rows.astype(BF16)

    @pl.when(step >= num_heads)
    def _():
        y_ref[...] = dot_nn(o_ref[...], wo_ref[...]).astype(BF16)


def final_attention(flags, q, ot, st, lse, keys, values, far, w_out):
    num_heads, width, tokens = ot.shape
    d_model = w_out.shape[1]
    ins = (q, ot, st, lse, *keys, *values, *far)
    use = (1, None, None, None, 1, 1, 1, 1, 2, 2, 3, 3)
    column = lambda h, flags: (0, jnp.maximum(h - num_heads, 0))
    return pl.pallas_call(
        lambda *refs: final_kernel(num_heads, *refs),
        grid_spec=pltpu.PrefetchScalarGridSpec(
            num_scalar_prefetch=1,
            grid=(num_heads + d_model // 256,),
            in_specs=[head_spec(a.shape, last=num_heads - 1, flag=flag) for a, flag in zip(ins, use)] + [pl.BlockSpec((w_out.shape[0], 256), column)],
            out_specs=pl.BlockSpec((tokens, 256), column),
            scratch_shapes=[pltpu.VMEM((tokens, num_heads * width), BF16), pltpu.VMEM((width, tokens // 4), BF16)],
        ),
        out_shape=jax.ShapeDtypeStruct((tokens, d_model), BF16),
        compiler_params=params(),
        cost_estimate=pl.CostEstimate(flops=3 * 10 ** 10, bytes_accessed=6 * 10 ** 7, transcendentals=5 * 10 ** 6),
        name="final_attention",
    )(flags, *ins, w_out)


def solution(mesh):
    row_spec = P(('dp', 'seq'), None)
    swap = [(s, s ^ 1) for s in range(8)]
    next_chip = [(0, 2), (1, 3), (4, 6), (5, 7)]
    swap_upper = [(s, s ^ 1) for s in (2, 3, 6, 7)]
    from_first = [(0, 4), (1, 5)]
    from_second = [(2, 4), (3, 5)]
    swap_third = [(4, 5), (5, 4)]
    to_third = [(6, 4), (7, 5)]
    to_fourth = [(4, 6), (5, 7)]

    def send(array, pairs):
        return lax.ppermute(array, 'seq', pairs)

    def layer(hidden, w_query, w_key, w_value, w_out):
        tokens, d_model = hidden.shape
        num_heads, head_dim = w_query.shape[1:]
        index = lax.axis_index('seq')
        chip = index // 2
        flags = jnp.stack([index % 2, chip % 2, (chip == 2).astype(jnp.int32), (chip == 3).astype(jnp.int32)]).astype(jnp.int32)

        order = jnp.arange(CHUNK)
        perm = ((order % RUN) * CLASSES + order // RUN)[:, None] == order[None, :]
        x = jnp.einsum('pq,cqd->cpd', perm.astype(BF16), hidden.reshape(tokens // CHUNK, CHUNK, d_model),
                       preferred_element_type=F32).astype(BF16).reshape(tokens, d_model)

        def project(weight):
            return jnp.einsum('td,dhe->hte', x, weight, preferred_element_type=F32)

        def spread(packs):
            far_rows, quad_rows, pair_rows = packs
            first = send(far_rows, from_first)
            second = send(far_rows, from_second)
            quad = send(quad_rows, next_chip)
            pair = send(pair_rows, swap)
            swapped = send(first, swap_third), send(second, swap_third)
            return pair, (quad, send(quad, swap_upper)), (first, second, *swapped)

        k = project(w_key).astype(BF16)
        pair_k, quad_k, far_k = spread(pack(k, (1, 2, 4)))
        v = project(w_value).astype(BF16)
        pair_v, quad_v, far_v = spread(pack(v, (1, 2, 4)))
        q = (project(w_query) * head_dim ** -0.5).astype(BF16)
        q_far, = pack(q, (1,))
        q_later = send(q_far, to_third)

        early = 2
        state = local_attention(flags, q, k, v, pair_k, pair_v, 0, early, (), ())
        own_o, own_lse, later_o, later_lse = far_attention(flags, q_far, q_later, far_k, far_v, (state[2],))
        got_o, got_lse = send(later_o, to_fourth), send(later_lse, to_fourth)
        ot, st, lse, q_late = local_attention(flags, q, k, v, pair_k, pair_v, early, num_heads - early, state, (own_lse,))
        return final_attention(flags, q_late, ot, st, lse, quad_k, quad_v, (own_o, own_lse, got_o, got_lse),
                               w_out.reshape(num_heads * head_dim, d_model))

    return jax.shard_map(layer, mesh=mesh, in_specs=(row_spec, P(), P(), P(), P()), out_specs=row_spec, check_vma=False)
```
